32 devices in a mesh: sub: 8 (over z, core), sta: 4 (over y, x).
Axes of the slice: x: 2, y: 2, z: 4, core: 2. Of those that a mesh axis runs over, the one named last changes fastest.
Arguments:
- voltages: bfloat16 [8, 2, 64, 65536], P('sub', None, 'sta'), may hold values from -6 to 6
- beam_weights: bfloat16 [8, 2, 32, 64], P('sub'), may hold values from -0.5 to 0.5
- station_delays: int32 [64], P('sta'), may hold values from 0 to 16383
- dm_index: int32 [32, 1], P('sta'), may hold values from 1 to 8
Outputs:
- dedispersed: float32 [8, 2, 32, 1, 65536], P(None, None, None, None, ('sub', 'sta'))
- intensity: float32 [32, 1, 65536], P(None, None, ('sub', 'sta'))
The draws below stay inside these ranges and needn't reach their ends.
Inputs may be any that keep to these rules, and one draw needn't show every extreme that they name: `station_delays`: delays in whole samples. `dm_index`: dispersion measure in steps of 10.
All inputs are finite; a program needn't handle non-finite values.
Results may differ from the reference program's by a relative error of at most 0.0006.
Values may be sent and summed in bfloat16 or wider, within the bound.
A program may use at most 320 MiB of HBM per device.

```python
import jax
import jax.numpy as jnp
from jax import lax

STATIONS = 64
BEAMS = 32
DMS = 1
SAMPLES = 65536
SUBBANDS = 8


def set_ends(values, key, low, largest):
    extent = values.shape
    spot = [jax.random.randint(jax.random.fold_in(key, axis), (), 0, extent[axis]) for axis in range(len(extent))]
    values = values.at[tuple(spot)].set(low)
    longest = extent.index(max(extent))
    spot[longest] = (spot[longest] + 1) % extent[longest]
    return values.at[tuple(spot)].set(largest)


def block_scale(rng, shape, split, low, top_value):
    def one(axis_at, shards_of):
        heights = jax.random.uniform(jax.random.fold_in(jax.random.fold_in(rng, 6), axis_at), (shards_of,), jnp.float32, low / len(split), top_value / len(split))
        return jnp.repeat(jnp.exp(heights), shape[axis_at] // shards_of).reshape((-1,) + (1,) * (len(shape) - axis_at - 1))

    gain = one(*split[0])
    for cut in split[1:]:
        gain = gain * one(*cut)
    return gain


def bell_draw(own_key, dims, scale, limit, pieces=(), kind=jnp.bfloat16):
    drawn = jax.random.normal(own_key, dims, jnp.float32) * scale
    if len(pieces) > 0:
        drawn = block_scale(own_key, dims, pieces, -0.22, 0.18) * drawn
    return jnp.clip(drawn, min=-limit, max=limit).astype(kind)


def setup_inputs(seed: int = 0) -> dict:
    streams_of = jax.random.split(jax.random.key(seed), 5)
    voltages = bell_draw(streams_of[0], (SUBBANDS, 2, STATIONS, SAMPLES), 1.0, 6.0, ((0, 8), (2, 4)))
    beam_weights = bell_draw(streams_of[1], (SUBBANDS, 2, BEAMS, STATIONS), (2 * STATIONS) ** -0.5, 0.5, ((0, 8),))
    station_delays = set_ends(jax.random.randint(streams_of[2], (STATIONS,), 0, SAMPLES // 4), jax.random.fold_in(streams_of[2], 1), 0, (SAMPLES // 4) - 1).astype(jnp.int32)
    dm_index = set_ends(jax.random.randint(streams_of[3], (BEAMS, DMS), 1, 9), jax.random.fold_in(streams_of[3], 1), 1, 8).astype(jnp.int32)
    return dict(voltages=voltages, beam_weights=beam_weights, station_delays=station_delays, dm_index=dm_index)


TWO_PI = 6.283185307179586
DISPERSION = 4148808000.0
DM_STEP = 10.0
BASE_FREQ = 120.0
CHANNEL_WIDTH = 0.1953125


def chirp_base(subband, total_len):
    positions = jnp.arange(total_len, dtype=jnp.int32)
    signed_bin = jnp.where(positions < total_len // 2, positions, positions - total_len)
    offset = CHANNEL_WIDTH * signed_bin.astype(jnp.float32) / total_len
    centre = BASE_FREQ + CHANNEL_WIDTH * (subband.astype(jnp.float32) + 0.5)
    return TWO_PI * DISPERSION * offset * offset / (centre * centre * (centre + offset))


def reference(voltages, beam_weights, station_delays, dm_index):
    dm_value = DM_STEP * dm_index.astype(jnp.float32)

    def one_subband(inputs):
        subband, volts, weights = inputs
        shifted = jax.vmap(lambda rows, shift_by: jnp.roll(rows, shift_by, axis=-1), in_axes=(1, 0), out_axes=1)(volts, station_delays)
        real_part = jnp.dot(weights[0], shifted[0], preferred_element_type=jnp.float32) - jnp.dot(weights[1], shifted[1], preferred_element_type=jnp.float32)
        imag_part = jnp.dot(weights[0], shifted[1], preferred_element_type=jnp.float32) + jnp.dot(weights[1], shifted[0], preferred_element_type=jnp.float32)
        spectrum = jnp.fft.fft(lax.complex(real_part, imag_part), axis=-1)
        phase_table = dm_value[:, :, None] * chirp_base(subband, SAMPLES)[None, None, :]
        chirped = spectrum[:, None, :] * lax.complex(jnp.cos(phase_table), jnp.sin(phase_table))
        series = jnp.fft.ifft(chirped, axis=-1)
        return jnp.stack([jnp.real(series), jnp.imag(series)], axis=0)

    dedispersed = lax.map(one_subband, (jnp.arange(SUBBANDS, dtype=jnp.int32), voltages, beam_weights))
    intensity = jnp.mean(dedispersed[:, 0] * dedispersed[:, 0] + dedispersed[:, 1] * dedispersed[:, 1], axis=0)
    return dedispersed, intensity
```

```python
import functools

import jax
import jax.numpy as jnp
import numpy as np
from jax import lax
from jax.experimental import pallas as pl
from jax.experimental.pallas import tpu as pltpu
from jax.sharding import PartitionSpec as P


TWO_PI = 6.283185307179586
DISPERSION = 4148808000.0
DM_STEP = 10.0
BASE_FREQ = 120.0
CHANNEL_WIDTH = 0.1953125


def dft_tables(root_len):
    total_len = root_len * root_len
    product = np.outer(np.arange(root_len), np.arange(root_len))
    root_angle = 2 * np.pi * (product % root_len) / root_len
    cos_root, sin_root = np.cos(root_angle), np.sin(root_angle)
    left = np.block([[cos_root, sin_root], [-sin_root, cos_root]]).astype(np.float32)
    high = left.astype(jnp.bfloat16)
    low = (left - high.astype(np.float32)).astype(jnp.bfloat16)
    twist_angle = 2 * np.pi * product / total_len
    twist = np.stack([np.cos(twist_angle), np.sin(twist_angle)]).astype(np.float32)
    return np.stack([high, low]), np.stack([high.T, low.T]), twist


def chirp_base(subband, root_len, total_len):
    first = jnp.arange(root_len, dtype=jnp.int32)[:, None]
    second = jnp.arange(root_len, dtype=jnp.int32)[None, :]
    positions = first + root_len * second
    signed_bin = jnp.where(positions < total_len // 2, positions, positions - total_len)
    offset = (CHANNEL_WIDTH * signed_bin.astype(jnp.float32) / total_len)[None]
    centre = (BASE_FREQ + CHANNEL_WIDTH * (subband.astype(jnp.float32) + 0.5))[:, None, None]
    return TWO_PI * DISPERSION * offset * offset / (centre * centre * (centre + offset))


def shift_kernel(delay_ref, x_ref, out_ref, source, moved):
    rows, total_len = x_ref.shape[1:]
    blocks = total_len // 128
    pitch = source.shape[0] // (blocks + 16)
    def load(i, carry):
        for u in range(8):
            j = i * 8 + u
            source[pl.ds(j*pitch, rows), :] = x_ref[0, :, pl.ds(pl.multiple_of(j * 128, 128), 128)].astype(jnp.float32)
        return carry
    lax.fori_loop(0, blocks // 8, load, 0)
    for u in range(16):
        source[pl.ds((blocks + u) * pitch, rows), :] = source[pl.ds(u * pitch, rows), :]
    lane = lax.broadcasted_iota(jnp.int32, (8, 128), 1)
    for row in range(rows):
        delay = delay_ref[row]
        fine = delay & 127
        coarse = delay >> 7
        keep = lane < 128 - fine
        def chunk(i, carry):
            for u in range(32):
                j = i * (8*32) + u * 8
                start = (j - coarse - 1) & (blocks - 1)
                before = source[pl.ds(start * pitch + row, 8, stride=pitch), :]
                after = source[pl.ds((start + 1) * pitch + row, 8, stride=pitch), :]
                values = pltpu.roll(jnp.where(keep, after, before), fine, 1)
                moved[pl.ds(j * pitch + row, 8, stride=pitch), :] = values
            return carry
        lax.fori_loop(0, blocks // (8*32), chunk, 0)
    def store(i, carry):
        for u in range(8):
            j = i * 8 + u
            out_ref[j] = moved[pl.ds(j*pitch, rows), :].astype(out_ref.dtype)
        return carry
    lax.fori_loop(0, blocks // 8, store, 0)


def shift(volts, delays):
    parts, rows, total_len = volts.shape
    blocks = total_len // 128
    pitch = rows + 4
    return pl.pallas_call(
        shift_kernel,
        grid=(parts,),
        in_specs=[pl.BlockSpec(memory_space=pltpu.SMEM), pl.BlockSpec((1, rows, total_len), lambda i: (i, 0, 0))],
        out_specs=pl.BlockSpec((blocks, rows, 128), lambda i: (0, i, 0)),
        out_shape=jax.ShapeDtypeStruct((blocks, parts * rows, 128), volts.dtype),
        scratch_shapes=[pltpu.VMEM(((blocks + 16) * pitch, 128), jnp.float32), pltpu.VMEM((blocks * pitch, 128), jnp.float32)],
    )(delays, volts)


MESH = pl.DeviceIdType.MESH
PEAK = 32767.0


def peers(side, n_low, n_high):
    sub, sta = lax.axis_index("sub"), lax.axis_index("sta")
    high, low = sta // n_low, lax.rem(sta, n_low)
    along = (
        [(sub, high * n_low + lax.rem(low + k, n_low)) for k in range(1, n_low)],
        [(sub, lax.rem(high + k, n_high) * n_low + low) for k in range(1, n_high)],
    )
    return along[side], along[1 - side]


def quantize(values, ceiling):
    return jnp.round(values * (PEAK / jnp.maximum(ceiling, 1e-30))).astype(jnp.int32).astype(jnp.int16)


def dequantize(codes, ceiling):
    return codes.astype(jnp.int32).astype(jnp.float32) * (ceiling * (1.0 / PEAK))


def beams_kernel(n_low, n_high, chunks, volt_ref, w0_ref, w1_ref, out_ref, *scratch):
    got, partial, codes, landed, scale, scale_in = (scratch[2 * i : 2 * i + 2] for i in range(6))
    gather_send, gather_recv, sum_send, sum_recv, scale_send, scale_recv = (
        scratch[12 + 2 * i : 14 + 2 * i] for i in range(6)
    )
    weight_refs = (w0_ref, w1_ref)
    n_beams, root = out_ref.shape[1:3]
    half = root // 2
    pitch = partial[0].shape[1] // weight_refs[0].shape[0]
    blocks = volt_ref.shape[0] // 2 // chunks

    barrier = pltpu.get_barrier_semaphore()
    for peer in (*peers(0, n_low, n_high)[0], *peers(0, n_low, n_high)[1]):
        pl.semaphore_signal(barrier, inc=1, device_id=peer, device_id_type=MESH)
    pl.semaphore_wait(barrier, n_low + n_high - 2)

    gathers = {}
    for chunk in range(chunks):
        for side in range(2):
            for k, peer in enumerate(peers(side, n_low, n_high)[0]):
                copy = pltpu.make_async_remote_copy(
                    src_ref=volt_ref.at[pl.ds((side * chunks + chunk) * blocks, blocks)],
                    dst_ref=got[side].at[k, pl.ds(chunk * blocks, blocks)],
                    send_sem=gather_send[side].at[k, chunk],
                    recv_sem=gather_recv[side].at[k, chunk],
                    device_id=peer,
                    device_id_type=MESH,
                )
                copy.start()
                gathers[side, k, chunk] = copy

    for chunk in range(chunks):
        for side in range(2):
            members = len(peers(side, n_low, n_high)[0])
            for k in range(members):
                gathers[side, k, chunk].wait_recv()
            weights = weight_refs[side][...]

            def rows(i, carry):
                for u in range(8):
                    row = chunk * (blocks // 2) + i * 8 + u
                    own = side * (volt_ref.shape[0] // 2) + 2 * row
                    tall = [
                        jnp.concatenate([ref[at], ref[at + 1]], axis=1)
                        for ref, at in ((volt_ref, own), *((got[side].at[k], 2 * row) for k in range(members)))
                    ]
                    sums = jnp.dot(weights, jnp.concatenate(tall, axis=0), preferred_element_type=jnp.float32)
                    for lanes in range(2):
                        for base in range(0, weights.shape[0], 8):
                            partial[side][lanes, pl.ds(base * pitch + row, 8, stride=pitch), :] = sums[
                                base : base + 8, lanes * 128 : (lanes + 1) * 128
                            ]
                return carry

            lax.fori_loop(0, blocks // 16, rows, 0)

    def piece(side, k, part, beam, lanes):
        return partial[side][lanes, pl.ds(((k * 2 + part) * n_beams + beam) * pitch, half), :]

    for side in range(2):
        for k in range(len(peers(side, n_low, n_high)[1])):

            def encode(beam, carry):
                for lanes in range(2):
                    values = [piece(side, k + 1, part, beam, lanes) for part in range(2)]
                    ceiling = jnp.max(jnp.maximum(jnp.abs(values[0]), jnp.abs(values[1])), axis=0, keepdims=True)
                    scale[side][k, beam, lanes : lanes + 1, :] = ceiling
                    for part in range(2):
                        codes[side][k, beam, part, lanes] = quantize(values[part], ceiling)
                return carry

            lax.fori_loop(0, n_beams, encode, 0)

    scales = {}
    for side in range(2):
        for k, peer in enumerate(peers(side, n_low, n_high)[1]):
            scales[side, k] = pltpu.make_async_remote_copy(
                src_ref=scale[side].at[k],
                dst_ref=scale_in[side].at[k],
                send_sem=scale_send[side].at[k],
                recv_sem=scale_recv[side].at[k],
                device_id=peer,
                device_id_type=MESH,
            )
            scales[side, k].start()

    def exchange(side, k, beam):
        return pltpu.make_async_remote_copy(
            src_ref=codes[side].at[k, beam],
            dst_ref=landed[side].at[k, beam],
            send_sem=sum_send[side].at[k, beam],
            recv_sem=sum_recv[side].at[k, beam],
            device_id=peers(side, n_low, n_high)[1][k],
            device_id_type=MESH,
        )

    def each_exchange(beam, act):
        for side in range(2):
            for k in range(len(peers(side, n_low, n_high)[1])):
                act(exchange(side, k, beam))

    def launch(beam, carry):
        each_exchange(beam, lambda copy: copy.start())
        return carry

    lax.fori_loop(0, n_beams, launch, 0)
    for copy in scales.values():
        copy.wait_recv()

    def finish(beam, carry):
        each_exchange(beam, lambda copy: copy.wait_recv())
        for side in range(2):
            for lanes in range(2):
                for part in range(2):
                    total = piece(side, 0, part, beam, lanes)
                    for k in range(len(peers(side, n_low, n_high)[1])):
                        ceiling = scale_in[side][k, beam, lanes : lanes + 1, :]
                        total = total + dequantize(landed[side][k, beam, part, lanes], ceiling)
                    out_ref[part, beam, side * half : (side + 1) * half, lanes * 128 : (lanes + 1) * 128] = total
        return carry

    lax.fori_loop(0, n_beams, finish, 0)

    def drain(beam, carry):
        each_exchange(beam, lambda copy: copy.wait_send())
        return carry

    lax.fori_loop(0, n_beams, drain, 0)
    for copy in (*gathers.values(), *scales.values()):
        copy.wait_send()


def sum_beams(volts, weights, n_low, n_high, n_beams, root):
    blocks, depth, _ = volts.shape
    chunks = 4
    half = root // 2
    pitch = half + 4
    dma = pltpu.SemaphoreType.DMA
    groups = ((n_low, n_high), (n_high, n_low))
    per_side = lambda make: [make(*group) for group in groups]
    return pl.pallas_call(
        functools.partial(beams_kernel, n_low, n_high, chunks),
        in_specs=[pl.BlockSpec(memory_space=pltpu.VMEM)] * 3,
        out_specs=pl.BlockSpec(memory_space=pltpu.VMEM),
        out_shape=jax.ShapeDtypeStruct((2, n_beams, root, root), jnp.float32),
        scratch_shapes=[
            *per_side(lambda g, r: pltpu.VMEM((g - 1, blocks // 2, depth, 128), jnp.bfloat16)),
            *per_side(lambda g, r: pltpu.VMEM((2, r * 2 * n_beams * pitch, 128), jnp.float32)),
            *per_side(lambda g, r: pltpu.VMEM((r - 1, n_beams, 2, 2, half, 128), jnp.int16)),
            *per_side(lambda g, r: pltpu.VMEM((r - 1, n_beams, 2, 2, half, 128), jnp.int16)),
            *per_side(lambda g, r: pltpu.VMEM((r - 1, n_beams, 8, 128), jnp.float32)),
            *per_side(lambda g, r: pltpu.VMEM((r - 1, n_beams, 8, 128), jnp.float32)),
            *per_side(lambda g, r: dma((g - 1, chunks))),
            *per_side(lambda g, r: dma((g - 1, chunks))),
            *per_side(lambda g, r: dma((r - 1, n_beams))),
            *per_side(lambda g, r: dma((r - 1, n_beams))),
            *per_side(lambda g, r: dma((r - 1,))),
            *per_side(lambda g, r: dma((r - 1,))),
        ],
        compiler_params=pltpu.CompilerParams(
            collective_id=0, has_side_effects=True, vmem_limit_bytes=60 * 1024 * 1024
        ),
        cost_estimate=pl.CostEstimate(
            flops=8 * n_beams * depth * blocks * 128, bytes_accessed=2 * volts.size, transcendentals=0
        ),
    )(volts, *weights)


def order_weights(own_weights, n_low, n_high, n_beams):
    n_sta = n_low * n_high
    w_real, w_imag = own_weights[0], own_weights[1]
    full = jnp.stack([jnp.stack([w_real, -w_imag], axis=1), jnp.stack([w_imag, w_real], axis=1)])
    full = full.reshape(2, n_sta, n_beams, 2, n_sta, -1)
    sta = lax.axis_index("sta")
    high, low = sta // n_low, lax.rem(sta, n_low)
    in_row = lambda step, n: high * n_low + lax.rem(low + step * jnp.arange(n) + n, n)
    in_column = lambda step, n: lax.rem(high + step * jnp.arange(n) + n, n) * n_low + low
    out = []
    for beam_ids, station_ids in (
        (in_column(1, n_high), in_row(-1, n_low)),
        (in_row(1, n_low), in_column(-1, n_high)),
    ):
        chosen = jnp.take(jnp.take(full, beam_ids, axis=1), station_ids, axis=4)
        chosen = chosen.transpose(1, 0, 2, 4, 3, 5)
        out.append(chosen.reshape(chosen.shape[0] * 2 * n_beams, -1))
    return out


def split(values):
    high = values.astype(jnp.bfloat16)
    return high, (values - high.astype(jnp.float32)).astype(jnp.bfloat16)


def dot3(a_high, a_low, b_high, b_low):
    dot = functools.partial(jnp.dot, preferred_element_type=jnp.float32)
    return dot(a_high, b_high) + (dot(a_high, b_low) + dot(a_low, b_high))


def dedisperse_kernel(x_ref, h_real_ref, h_imag_ref, left_ref, right_ref, twist_ref, out_ref, flat):
    root = twist_ref.shape[1]
    half = root // 2
    cos_twist, sin_twist = twist_ref[0], twist_ref[1]
    x = x_ref[...].reshape(2 * root, root)
    a = dot3(left_ref[0], left_ref[1], *split(x))
    a_real, a_imag = a[:root], a[root:]
    b = jnp.concatenate(
        [a_real * cos_twist + a_imag * sin_twist, a_imag * cos_twist - a_real * sin_twist], axis=1
    )
    s = dot3(*split(b), right_ref[0], right_ref[1])
    s_real, s_imag = s[:, :root], s[:, root:]
    h_real, h_imag = h_real_ref[0], h_imag_ref[0]
    c = jnp.concatenate([s_real * h_real - s_imag * h_imag, s_real * h_imag + s_imag * h_real], axis=1)
    d = dot3(*split(c), left_ref[0], left_ref[1])
    d_real, d_imag = d[:, :root], d[:, root:]
    e = jnp.concatenate(
        [d_real * cos_twist - d_imag * sin_twist, d_imag * cos_twist + d_real * sin_twist], axis=0
    )
    out = dot3(right_ref[0], right_ref[1], *split(e)) * (1.0 / (root * root))
    for part in range(2):
        for side in range(2):
            flat[pl.ds(side, root, 2), :] = out[part * root : (part + 1) * root, side * half : (side + 1) * half]
        out_ref[:, part, 0] = flat[...].reshape(out_ref.shape[0], out_ref.shape[3], half)


def dedisperse(beams, h_real, h_imag, n_dev):
    _, n_beams, root, _ = beams.shape
    left, right, twist = dft_tables(root)
    rows = 2 * root // n_dev
    whole = lambda shape: pl.BlockSpec(shape, lambda b: (0,) * len(shape))
    own = pl.BlockSpec((1, root, root), lambda b: (b, 0, 0))
    return pl.pallas_call(
        dedisperse_kernel,
        grid=(n_beams,),
        in_specs=[
            pl.BlockSpec((2, 1, root, root), lambda b: (0, b, 0, 0)),
            own,
            own,
            whole(left.shape),
            whole(right.shape),
            whole(twist.shape),
        ],
        out_specs=pl.BlockSpec((n_dev, 2, 1, rows, root // 2), lambda b: (0, 0, b, 0, 0)),
        out_shape=jax.ShapeDtypeStruct((n_dev, 2, n_beams, rows, root // 2), jnp.float32),
        scratch_shapes=[pltpu.VMEM((2 * root, root // 2), jnp.float32)],
        cost_estimate=pl.CostEstimate(
            flops=96 * n_beams * root**3, bytes_accessed=24 * n_beams * root**2, transcendentals=0
        ),
    )(beams, h_real, h_imag, left, right, twist)


def shards(voltages, beam_weights, station_delays, dm_index):
    sub_dev = voltages.shape[0]
    total_len = voltages.shape[3]
    local_beams = dm_index.shape[0]
    trials = dm_index.shape[1]
    root_len = int(round(total_len**0.5))
    n_sub = lax.axis_size("sub")
    n_sta = lax.axis_size("sta")
    n_dev = n_sub * n_sta
    assert sub_dev == 1 and trials == 1 and root_len * root_len == total_len
    shifted = shift(voltages[0], station_delays)
    n_low = 2 if n_sta % 2 == 0 else 1
    n_high = n_sta // n_low
    weights = order_weights(beam_weights[0], n_low, n_high, local_beams)
    beams = sum_beams(shifted, weights, n_low, n_high, local_beams, root_len)
    subband = lax.axis_index("sub") + jnp.arange(1, dtype=jnp.int32)
    base_phase = chirp_base(subband, root_len, total_len)
    dm_value = DM_STEP * dm_index.astype(jnp.float32)
    phase_table = dm_value[:, :, None] * base_phase
    sent = dedisperse(beams, jnp.cos(phase_table), jnp.sin(phase_table), n_dev)
    power = jnp.mean(beams[0] * beams[0] + beams[1] * beams[1], axis=(1, 2))
    rms = jnp.where(power > 0, jnp.sqrt(power), 1.0)
    gain = 32768.0 / root_len / rms
    undo = lax.all_gather(rms * (root_len / 32768.0), ("sub", "sta"), axis=0)
    sent = (sent * gain[None, None, :, None, None]).astype(jnp.float16)
    moved = lax.all_to_all(sent, ("sub", "sta"), split_axis=0, concat_axis=0, tiled=True)
    moved = moved.astype(jnp.float32) * undo[:, None, :, None, None]
    moved = moved.reshape(n_sub, n_sta, *moved.shape[1:]).transpose(0, 2, 1, 3, 4, 5)
    moved = moved.reshape(n_sub, 2, n_sta * local_beams, *moved.shape[4:])
    intensity = jnp.mean(moved[:, 0] * moved[:, 0] + moved[:, 1] * moved[:, 1], axis=0)
    return (moved.reshape(*moved.shape[:3], 1, -1), intensity.reshape(intensity.shape[0], 1, -1))


def solution(mesh):
    return jax.shard_map(
        shards,
        mesh=mesh,
        in_specs=(
            P("sub", None, "sta", None),
            P("sub", None, None, None),
            P("sta"),
            P("sta", None),
        ),
        out_specs=(P(None, None, None, None, ("sub", "sta")), P(None, None, ("sub", "sta"))),
        check_vma=False,
    )
```

```python
import functools

import jax
import jax.numpy as jnp
import numpy as np
from jax import lax
from jax.experimental import pallas as pl
from jax.experimental.pallas import tpu as pltpu
from jax.sharding import PartitionSpec as P


TWO_PI = 6.283185307179586
DISPERSION = 4148808000.0
DM_STEP = 10.0
BASE_FREQ = 120.0
CHANNEL_WIDTH = 0.1953125


def dft_tables(root_len):
    total_len = root_len * root_len
    product = np.outer(np.arange(root_len), np.arange(root_len))
    root_angle = 2 * np.pi * (product % root_len) / root_len
    cos_root, sin_root = np.cos(root_angle), np.sin(root_angle)
    left = np.block([[cos_root, sin_root], [-sin_root, cos_root]]).astype(np.float32)
    high = left.astype(jnp.bfloat16)
    low = (left - high.astype(np.float32)).astype(jnp.bfloat16)
    twist_angle = 2 * np.pi * product / total_len
    twist = np.stack([np.cos(twist_angle), np.sin(twist_angle)]).astype(np.float32)
    return np.stack([high, low]), np.stack([high.T, low.T]), twist


def chirp_base(subband, root_len, total_len):
    first = jnp.arange(root_len, dtype=jnp.int32)[:, None]
    second = jnp.arange(root_len, dtype=jnp.int32)[None, :]
    positions = first + root_len * second
    signed_bin = jnp.where(positions < total_len // 2, positions, positions - total_len)
    offset = (CHANNEL_WIDTH * signed_bin.astype(jnp.float32) / total_len)[None]
    centre = (BASE_FREQ + CHANNEL_WIDTH * (subband.astype(jnp.float32) + 0.5))[:, None, None]
    return TWO_PI * DISPERSION * offset * offset / (centre * centre * (centre + offset))


def shift_kernel(delay_ref, x_ref, out_ref, source, moved):
    rows, total_len = x_ref.shape[1:]
    blocks = total_len // 128
    pitch = source.shape[0] // (blocks + 16)
    def load(i, carry):
        for u in range(8):
            j = i * 8 + u
            source[pl.ds(j*pitch, rows), :] = x_ref[0, :, pl.ds(pl.multiple_of(j * 128, 128), 128)].astype(jnp.float32)
        return carry
    lax.fori_loop(0, blocks // 8, load, 0)
    for u in range(16):
        source[pl.ds((blocks + u) * pitch, rows), :] = source[pl.ds(u * pitch, rows), :]
    lane = lax.broadcasted_iota(jnp.int32, (8, 128), 1)
    for row in range(rows):
        delay = delay_ref[row]
        fine = delay & 127
        coarse = delay >> 7
        keep = lane < 128 - fine
        def chunk(i, carry):
            for u in range(32):
                j = i * (8*32) + u * 8
                start = (j - coarse - 1) & (blocks - 1)
                before = source[pl.ds(start * pitch + row, 8, stride=pitch), :]
                after = source[pl.ds((start + 1) * pitch + row, 8, stride=pitch), :]
                values = pltpu.roll(jnp.where(keep, after, before), fine, 1)
                moved[pl.ds(j * pitch + row, 8, stride=pitch), :] = values
            return carry
        lax.fori_loop(0, blocks // (8*32), chunk, 0)
    def store(i, carry):
        for u in range(8):
            j = i * 8 + u
            out_ref[j] = moved[pl.ds(j*pitch, rows), :].astype(out_ref.dtype)
        return carry
    lax.fori_loop(0, blocks // 8, store, 0)


def shift(volts, delays):
    parts, rows, total_len = volts.shape
    blocks = total_len // 128
    pitch = rows + 4
    return pl.pallas_call(
        shift_kernel,
        grid=(parts,),
        in_specs=[pl.BlockSpec(memory_space=pltpu.SMEM), pl.BlockSpec((1, rows, total_len), lambda i: (i, 0, 0))],
        out_specs=pl.BlockSpec((blocks, rows, 128), lambda i: (0, i, 0)),
        out_shape=jax.ShapeDtypeStruct((blocks, parts * rows, 128), volts.dtype),
        scratch_shapes=[pltpu.VMEM(((blocks + 16) * pitch, 128), jnp.float32), pltpu.VMEM((blocks * pitch, 128), jnp.float32)],
    )(delays, volts)


def split(values):
    high = values.astype(jnp.bfloat16)
    return high, (values - high.astype(jnp.float32)).astype(jnp.bfloat16)


def dot3(a_high, a_low, b_high, b_low):
    dot = functools.partial(jnp.dot, preferred_element_type=jnp.float32)
    return dot(a_high, b_high) + (dot(a_high, b_low) + dot(a_low, b_high))


MESH = pl.DeviceIdType.MESH
PEAK = 32767.0


def peers(side, n_low, n_high):
    sub, sta = lax.axis_index("sub"), lax.axis_index("sta")
    high, low = sta // n_low, lax.rem(sta, n_low)
    along = (
        [(sub, high * n_low + lax.rem(low + k, n_low)) for k in range(1, n_low)],
        [(sub, lax.rem(high + k, n_high) * n_low + low) for k in range(1, n_high)],
    )
    return along[side], along[1 - side]


def quantize(values, ceiling):
    return jnp.round(values * (PEAK / jnp.maximum(ceiling, 1e-30))).astype(jnp.int32).astype(jnp.int16)


def dequantize(codes, ceiling):
    return codes.astype(jnp.int32).astype(jnp.float32) * (ceiling * (1.0 / PEAK))


def turn(phase):
    count = jnp.round(phase * 0.6366197723675814)
    rest = ((phase - count * 1.5703125) - count * 4.837512969970703125e-4) - count * 7.54978995489188216e-8
    square = rest * rest
    sine = rest + rest * square * (
        (-1.9515295891e-4 * square + 8.3321608736e-3) * square - 1.6666654611e-1
    )
    cosine = (1.0 - 0.5 * square) + square * square * (
        (2.443315711809948e-5 * square - 1.388731625493765e-3) * square + 4.166664568298827e-2
    )
    quarter = count.astype(jnp.int32)
    odd = (quarter & 1) == 1
    real, imag = jnp.where(odd, sine, cosine), jnp.where(odd, cosine, sine)
    real = jnp.where(((quarter + 1) & 2) == 2, -real, real)
    imag = jnp.where((quarter & 2) == 2, -imag, imag)
    return real, imag


def disperse(x, h_real, h_imag, left_ref, right_ref, twist_ref):
    root = twist_ref.shape[1]
    cos_twist, sin_twist = twist_ref[0], twist_ref[1]
    a = dot3(left_ref[0], left_ref[1], *split(x))
    a_real, a_imag = a[:root], a[root:]
    b = jnp.concatenate(
        [a_real * cos_twist + a_imag * sin_twist, a_imag * cos_twist - a_real * sin_twist], axis=1
    )
    s = dot3(*split(b), right_ref[0], right_ref[1])
    s_real, s_imag = s[:, :root], s[:, root:]
    c = jnp.concatenate([s_real * h_real - s_imag * h_imag, s_real * h_imag + s_imag * h_real], axis=1)
    d = dot3(*split(c), left_ref[0], left_ref[1])
    d_real, d_imag = d[:, :root], d[:, root:]
    e = jnp.concatenate(
        [d_real * cos_twist - d_imag * sin_twist, d_imag * cos_twist + d_real * sin_twist], axis=0
    )
    return dot3(right_ref[0], right_ref[1], *split(e)) * (1.0 / (root * root))


def series_kernel(
    n_low,
    n_high,
    chunks,
    dm_ref,
    volt_ref,
    w0_ref,
    w1_ref,
    base_ref,
    left_ref,
    right_ref,
    twist_ref,
    out_ref,
    peak_ref,
    *scratch,
):
    got, partial, codes, landed, scale, scale_in = (scratch[2 * i : 2 * i + 2] for i in range(6))
    gather_send, gather_recv, sum_send, sum_recv, scale_send, scale_recv = (
        scratch[12 + 2 * i : 14 + 2 * i] for i in range(6)
    )
    chirp, flat, ready, ready_peak, middle, middle_peak = scratch[24:30]
    move_send, move_recv, peak_send, peak_recv, pass_send, pass_recv, last_send, last_recv, own_sem = scratch[30:]
    weight_refs = (w0_ref, w1_ref)
    n_sta, n_beams, n_sub, _, rows_out, _ = out_ref.shape
    root = twist_ref.shape[1]
    n_dev = n_sub * n_sta
    sub, sta = lax.axis_index("sub"), lax.axis_index("sta")
    sub_peer = lambda k: lax.rem(sub + k, n_sub)
    sta_peer = lambda k: lax.rem(sta + k, n_sta)
    half = root // 2
    pitch = partial[0].shape[1] // weight_refs[0].shape[0]
    blocks = volt_ref.shape[0] // 2 // chunks

    barrier = pltpu.get_barrier_semaphore()

    for k in range(1, n_sub):
        pl.semaphore_signal(barrier, inc=1, device_id=(sub_peer(k), sta), device_id_type=MESH)
    for k in range(1, n_sta):
        pl.semaphore_signal(barrier, inc=1, device_id=(sub, sta_peer(k)), device_id_type=MESH)
    pl.semaphore_wait(barrier, n_sub + n_sta - 2)

    gathers = {}
    for chunk in range(chunks):
        for side in range(2):
            for k, peer in enumerate(peers(side, n_low, n_high)[0]):
                copy = pltpu.make_async_remote_copy(
                    src_ref=volt_ref.at[pl.ds((side * chunks + chunk) * blocks, blocks)],
                    dst_ref=got[side].at[k, pl.ds(chunk * blocks, blocks)],
                    send_sem=gather_send[side].at[k, chunk],
                    recv_sem=gather_recv[side].at[k, chunk],
                    device_id=peer,
                    device_id_type=MESH,
                )
                copy.start()
                gathers[side, k, chunk] = copy

    def turns(beam, carry):
        measure = DM_STEP * dm_ref[beam, 0].astype(jnp.float32)
        for part in range(0, root, 64):
            chirp[beam, 0, part : part + 64], chirp[beam, 1, part : part + 64] = turn(
                measure * base_ref[0, part : part + 64]
            )
        return carry

    lax.fori_loop(0, n_beams, turns, 0)

    for chunk in range(chunks):
        for side in range(2):
            members = len(peers(side, n_low, n_high)[0])
            for k in range(members):
                gathers[side, k, chunk].wait_recv()
            weights = weight_refs[side][...]

            def rows(i, carry):
                for u in range(8):
                    row = chunk * (blocks // 2) + i * 8 + u
                    own = side * (volt_ref.shape[0] // 2) + 2 * row
                    tall = [
                        jnp.concatenate([ref[at], ref[at + 1]], axis=1)
                        for ref, at in ((volt_ref, own), *((got[side].at[k], 2 * row) for k in range(members)))
                    ]
                    sums = jnp.dot(weights, jnp.concatenate(tall, axis=0), preferred_element_type=jnp.float32)
                    for lanes in range(2):
                        for base in range(0, weights.shape[0], 8):
                            partial[side][lanes, pl.ds(base * pitch + row, 8, stride=pitch), :] = sums[
                                base : base + 8, lanes * 128 : (lanes + 1) * 128
                            ]
                return carry

            lax.fori_loop(0, blocks // 16, rows, 0)

    def piece(side, k, part, beam, lanes):
        return partial[side][lanes, pl.ds(((k * 2 + part) * n_beams + beam) * pitch, half), :]

    for side in range(2):
        for k in range(len(peers(side, n_low, n_high)[1])):

            def encode(beam, carry):
                for lanes in range(2):
                    values = [piece(side, k + 1, part, beam, lanes) for part in range(2)]
                    ceiling = jnp.max(jnp.maximum(jnp.abs(values[0]), jnp.abs(values[1])), axis=0, keepdims=True)
                    scale[side][k, beam, lanes : lanes + 1, :] = ceiling
                    for part in range(2):
                        codes[side][k, beam, part, lanes] = quantize(values[part], ceiling)
                return carry

            lax.fori_loop(0, n_beams, encode, 0)

    scales = {}
    for side in range(2):
        for k, peer in enumerate(peers(side, n_low, n_high)[1]):
            scales[side, k] = pltpu.make_async_remote_copy(
                src_ref=scale[side].at[k],
                dst_ref=scale_in[side].at[k],
                send_sem=scale_send[side].at[k],
                recv_sem=scale_recv[side].at[k],
                device_id=peer,
                device_id_type=MESH,
            )
            scales[side, k].start()

    def exchange(side, k, beam):
        return pltpu.make_async_remote_copy(
            src_ref=codes[side].at[k, beam],
            dst_ref=landed[side].at[k, beam],
            send_sem=sum_send[side].at[k, beam],
            recv_sem=sum_recv[side].at[k, beam],
            device_id=peers(side, n_low, n_high)[1][k],
            device_id_type=MESH,
        )

    def each_exchange(beam, act):
        for side in range(2):
            for k in range(len(peers(side, n_low, n_high)[1])):
                act(exchange(side, k, beam))

    def launch(beam, carry):
        each_exchange(beam, lambda copy: copy.start())
        return carry

    lax.fori_loop(0, n_beams, launch, 0)
    for copy in scales.values():
        copy.wait_recv()

    def move(beam, k):
        return pltpu.make_async_remote_copy(
            src_ref=ready.at[sub_peer(k), beam],
            dst_ref=middle.at[beam, sub],
            send_sem=move_send.at[beam, k - 1],
            recv_sem=move_recv.at[beam, k - 1],
            device_id=(sub_peer(k), sta),
            device_id_type=MESH,
        )

    def move_peak(k):
        return pltpu.make_async_remote_copy(
            src_ref=ready_peak,
            dst_ref=middle_peak.at[sub],
            send_sem=peak_send.at[k - 1],
            recv_sem=peak_recv.at[k - 1],
            device_id=(sub_peer(k), sta),
            device_id_type=MESH,
        )

    def forward(beam, k):
        return pltpu.make_async_remote_copy(
            src_ref=middle.at[beam, :, sta_peer(k)],
            dst_ref=out_ref.at[sta, beam],
            send_sem=pass_send.at[beam, k - 1],
            recv_sem=pass_recv.at[beam, k - 1],
            device_id=(sub, sta_peer(k)),
            device_id_type=MESH,
        )

    def forward_peak(k):
        return pltpu.make_async_remote_copy(
            src_ref=middle_peak,
            dst_ref=peak_ref.at[sta],
            send_sem=last_send.at[k - 1],
            recv_sem=last_recv.at[k - 1],
            device_id=(sub, sta_peer(k)),
            device_id_type=MESH,
        )

    def keep(beam):
        return pltpu.make_async_copy(middle.at[beam, :, sta], out_ref.at[sta, beam], own_sem.at[beam])

    def finish(beam, carry):
        each_exchange(beam, lambda copy: copy.wait_recv())
        quarters = []
        for part in range(2):
            for side in range(2):
                pair = []
                for lanes in range(2):
                    total = piece(side, 0, part, beam, lanes)
                    for k in range(len(peers(side, n_low, n_high)[1])):
                        ceiling = scale_in[side][k, beam, lanes : lanes + 1, :]
                        total = total + dequantize(landed[side][k, beam, part, lanes], ceiling)
                    pair.append(total)
                quarters.append(jnp.concatenate(pair, axis=1))
        x = jnp.concatenate(quarters, axis=0)
        series = disperse(x, chirp[beam, 0], chirp[beam, 1], left_ref, right_ref, twist_ref)
        for part in range(2):
            for lanes in range(2):
                flat[part, pl.ds(lanes, root, 2), :] = series[
                    part * root : (part + 1) * root, lanes * half : (lanes + 1) * half
                ]
        values = [flat[part] for part in range(2)]
        ceiling = jnp.max(jnp.maximum(jnp.abs(values[0]), jnp.abs(values[1])), axis=0, keepdims=True)
        ready_peak[pl.ds(beam, 1), :] = ceiling
        for part in range(2):
            ready[:, beam, :, part] = quantize(values[part], ceiling).reshape(n_sub, n_sta, rows_out, half)
        middle[beam, sub] = ready[sub, beam]
        for k in range(1, n_sub):
            move(beam, k).start()
        return carry

    lax.fori_loop(0, n_beams, finish, 0)
    middle_peak[sub] = ready_peak[...]
    for k in range(1, n_sub):
        move_peak(k).start()

    def spread(beam, carry):
        for k in range(1, n_sub):
            move(beam, k).wait_recv()
        for k in range(1, n_sta):
            forward(beam, k).start()
        keep(beam).start()
        return carry

    lax.fori_loop(0, n_beams, spread, 0)
    for k in range(1, n_sub):
        move_peak(k).wait_recv()
    for k in range(1, n_sta):
        forward_peak(k).start()
    own_peak = pltpu.make_async_copy(middle_peak, peak_ref.at[sta], own_sem.at[n_beams])
    own_peak.start()

    def drain(beam, carry):
        each_exchange(beam, lambda copy: copy.wait_send())
        return carry

    lax.fori_loop(0, n_beams, drain, 0)
    for copy in (*gathers.values(), *scales.values()):
        copy.wait_send()
    own_peak.wait()
    for k in range(1, n_sub):
        move_peak(k).wait_send()
    for k in range(1, n_sta):
        forward_peak(k).wait()

    def settle(beam, carry):
        keep(beam).wait()
        for k in range(1, n_sub):
            move(beam, k).wait_send()
        for k in range(1, n_sta):
            forward(beam, k).wait()
        return carry

    lax.fori_loop(0, n_beams, settle, 0)


def make_series(dm_index, volts, weights, base_phase, n_low, n_high, n_sub, root):
    blocks, depth, _ = volts.shape
    chunks = 4
    n_beams = dm_index.shape[0]
    half = root // 2
    n_sta = n_low * n_high
    rows_out = 2 * root // (n_sub * n_sta)
    tables = dft_tables(root)
    vmem = pl.BlockSpec(memory_space=pltpu.VMEM)
    hbm = pl.BlockSpec(memory_space=pltpu.HBM)
    pitch = half + 4
    dma = pltpu.SemaphoreType.DMA
    groups = ((n_low, n_high), (n_high, n_low))
    per_side = lambda make: [make(*group) for group in groups]
    return pl.pallas_call(
        functools.partial(series_kernel, n_low, n_high, chunks),
        in_specs=[pl.BlockSpec(memory_space=pltpu.SMEM), *[vmem] * 7],
        out_specs=(hbm, hbm),
        out_shape=(
            jax.ShapeDtypeStruct((n_sta, n_beams, n_sub, 2, rows_out, 128), jnp.int16),
            jax.ShapeDtypeStruct((n_sta, n_sub, n_beams, 128), jnp.float32),
        ),
        scratch_shapes=[
            *per_side(lambda g, r: pltpu.VMEM((g - 1, blocks // 2, depth, 128), jnp.bfloat16)),
            *per_side(lambda g, r: pltpu.VMEM((2, r * 2 * n_beams * pitch, 128), jnp.float32)),
            *per_side(lambda g, r: pltpu.VMEM((r - 1, n_beams, 2, 2, half, 128), jnp.int16)),
            *per_side(lambda g, r: pltpu.VMEM((r - 1, n_beams, 2, 2, half, 128), jnp.int16)),
            *per_side(lambda g, r: pltpu.VMEM((r - 1, n_beams, 8, 128), jnp.float32)),
            *per_side(lambda g, r: pltpu.VMEM((r - 1, n_beams, 8, 128), jnp.float32)),
            *per_side(lambda g, r: dma((g - 1, chunks))),
            *per_side(lambda g, r: dma((g - 1, chunks))),
            *per_side(lambda g, r: dma((r - 1, n_beams))),
            *per_side(lambda g, r: dma((r - 1, n_beams))),
            *per_side(lambda g, r: dma((r - 1,))),
            *per_side(lambda g, r: dma((r - 1,))),
            pltpu.VMEM((n_beams, 2, root, root), jnp.float32),
            pltpu.VMEM((2, 2 * root, 128), jnp.float32),
            pltpu.VMEM((n_sub, n_beams, n_sta, 2, rows_out, 128), jnp.int16),
            pltpu.VMEM((n_beams, 128), jnp.float32),
            pltpu.VMEM((n_beams, n_sub, n_sta, 2, rows_out, 128), jnp.int16),
            pltpu.VMEM((n_sub, n_beams, 128), jnp.float32),
            dma((n_beams, n_sub - 1)),
            dma((n_beams, n_sub - 1)),
            dma((n_sub - 1,)),
            dma((n_sub - 1,)),
            dma((n_beams, n_sta - 1)),
            dma((n_beams, n_sta - 1)),
            dma((n_sta - 1,)),
            dma((n_sta - 1,)),
            dma((n_beams + 1,)),
        ],
        compiler_params=pltpu.CompilerParams(
            collective_id=0, has_side_effects=True, vmem_limit_bytes=60 * 1024 * 1024
        ),
        cost_estimate=pl.CostEstimate(
            flops=8 * n_beams * depth * blocks * 128, bytes_accessed=2 * volts.size, transcendentals=0
        ),
    )(dm_index, volts, *weights, base_phase, *tables)


def order_weights(own_weights, n_low, n_high, n_beams):
    n_sta = n_low * n_high
    w_real, w_imag = own_weights[0], own_weights[1]
    full = jnp.stack([jnp.stack([w_real, -w_imag], axis=1), jnp.stack([w_imag, w_real], axis=1)])
    full = full.reshape(2, n_sta, n_beams, 2, n_sta, -1)
    sta = lax.axis_index("sta")
    high, low = sta // n_low, lax.rem(sta, n_low)
    in_row = lambda step, n: high * n_low + lax.rem(low + step * jnp.arange(n) + n, n)
    in_column = lambda step, n: lax.rem(high + step * jnp.arange(n) + n, n) * n_low + low
    out = []
    for beam_ids, station_ids in (
        (in_column(1, n_high), in_row(-1, n_low)),
        (in_row(1, n_low), in_column(-1, n_high)),
    ):
        chosen = jnp.take(jnp.take(full, beam_ids, axis=1), station_ids, axis=4)
        chosen = chosen.transpose(1, 0, 2, 4, 3, 5)
        out.append(chosen.reshape(chosen.shape[0] * 2 * n_beams, -1))
    return out


def shards(voltages, beam_weights, station_delays, dm_index):
    sub_dev = voltages.shape[0]
    total_len = voltages.shape[3]
    local_beams = dm_index.shape[0]
    trials = dm_index.shape[1]
    root_len = int(round(total_len**0.5))
    n_sub = lax.axis_size("sub")
    n_sta = lax.axis_size("sta")
    assert sub_dev == 1 and trials == 1 and root_len * root_len == total_len
    n_low = 2 if n_sta % 2 == 0 else 1
    n_high = n_sta // n_low
    shifted = shift(voltages[0], station_delays)
    weights = order_weights(beam_weights[0], n_low, n_high, local_beams)
    subband = lax.axis_index("sub") + jnp.arange(1, dtype=jnp.int32)
    base_phase = chirp_base(subband, root_len, total_len)
    codes, peak = make_series(dm_index, shifted, weights, base_phase, n_low, n_high, n_sub, root_len)
    peak = peak.transpose(1, 0, 2, 3)[:, None, :, :, None, :]
    moved = dequantize(codes.transpose(2, 3, 0, 1, 4, 5), peak)
    moved = moved.reshape(n_sub, 2, n_sta * local_beams, *moved.shape[4:])
    intensity = jnp.mean(moved[:, 0] * moved[:, 0] + moved[:, 1] * moved[:, 1], axis=0)
    return (moved.reshape(*moved.shape[:3], 1, -1), intensity.reshape(intensity.shape[0], 1, -1))


def solution(mesh):
    return jax.shard_map(
        shards,
        mesh=mesh,
        in_specs=(
            P("sub", None, "sta", None),
            P("sub", None, None, None),
            P("sta"),
            P("sta", None),
        ),
        out_specs=(P(None, None, None, None, ("sub", "sta")), P(None, None, ("sub", "sta"))),
        check_vma=False,
    )
```

```python
import functools

import jax
import jax.numpy as jnp
import numpy as np
from jax import lax
from jax.experimental import pallas as pl
from jax.experimental.pallas import tpu as pltpu
from jax.sharding import PartitionSpec as P


TWO_PI = 6.283185307179586
DISPERSION = 4148808000.0
DM_STEP = 10.0
BASE_FREQ = 120.0
CHANNEL_WIDTH = 0.1953125


def dft_tables(root_len):
    total_len = root_len * root_len
    product = np.outer(np.arange(root_len), np.arange(root_len))
    root_angle = 2 * np.pi * (product % root_len) / root_len
    cos_root, sin_root = np.cos(root_angle), np.sin(root_angle)
    left = np.block([[cos_root, sin_root], [-sin_root, cos_root]]).astype(np.float32)
    high = left.astype(jnp.bfloat16)
    low = (left - high.astype(np.float32)).astype(jnp.bfloat16)
    twist_angle = 2 * np.pi * product / total_len
    twist = np.stack([np.cos(twist_angle), np.sin(twist_angle)]).astype(np.float32)
    return np.stack([high, low]), np.stack([high.T, low.T]), twist


def chirp_base(subband, root_len, total_len):
    first = jnp.arange(root_len, dtype=jnp.int32)[:, None]
    second = jnp.arange(root_len, dtype=jnp.int32)[None, :]
    positions = first + root_len * second
    signed_bin = jnp.where(positions < total_len // 2, positions, positions - total_len)
    offset = (CHANNEL_WIDTH * signed_bin.astype(jnp.float32) / total_len)[None]
    centre = (BASE_FREQ + CHANNEL_WIDTH * (subband.astype(jnp.float32) + 0.5))[:, None, None]
    return TWO_PI * DISPERSION * offset * offset / (centre * centre * (centre + offset))


def split(values):
    high = values.astype(jnp.bfloat16)
    return high, (values - high.astype(jnp.float32)).astype(jnp.bfloat16)


def dot3(a_high, a_low, b_high, b_low):
    dot = functools.partial(jnp.dot, preferred_element_type=jnp.float32)
    return dot(a_high, b_high) + (dot(a_high, b_low) + dot(a_low, b_high))


MESH = pl.DeviceIdType.MESH
PEAK = 32767.0


def peers(side, n_low, n_high):
    sub, sta = lax.axis_index("sub"), lax.axis_index("sta")
    high, low = sta // n_low, lax.rem(sta, n_low)
    along = (
        [(sub, high * n_low + lax.rem(low + k, n_low)) for k in range(1, n_low)],
        [(sub, lax.rem(high + k, n_high) * n_low + low) for k in range(1, n_high)],
    )
    return along[side], along[1 - side]


def quantize(values, ceiling):
    return jnp.round(values * (PEAK / jnp.maximum(ceiling, 1e-30))).astype(jnp.int32).astype(jnp.int16)


def dequantize(codes, ceiling):
    return codes.astype(jnp.int32).astype(jnp.float32) * (ceiling * (1.0 / PEAK))


def turn(phase):
    count = jnp.round(phase * 0.6366197723675814)
    rest = ((phase - count * 1.5703125) - count * 4.837512969970703125e-4) - count * 7.54978995489188216e-8
    square = rest * rest
    sine = rest + rest * square * (
        (-1.9515295891e-4 * square + 8.3321608736e-3) * square - 1.6666654611e-1
    )
    cosine = (1.0 - 0.5 * square) + square * square * (
        (2.443315711809948e-5 * square - 1.388731625493765e-3) * square + 4.166664568298827e-2
    )
    quarter = count.astype(jnp.int32)
    odd = (quarter & 1) == 1
    real, imag = jnp.where(odd, sine, cosine), jnp.where(odd, cosine, sine)
    real = jnp.where(((quarter + 1) & 2) == 2, -real, real)
    imag = jnp.where((quarter & 2) == 2, -imag, imag)
    return real, imag


def disperse(x, h_real, h_imag, left_ref, right_ref, twist_ref):
    root = twist_ref.shape[1]
    cos_twist, sin_twist = twist_ref[0], twist_ref[1]
    a = dot3(left_ref[0], left_ref[1], *split(x))
    a_real, a_imag = a[:root], a[root:]
    b = jnp.concatenate(
        [a_real * cos_twist + a_imag * sin_twist, a_imag * cos_twist - a_real * sin_twist], axis=1
    )
    s = dot3(*split(b), right_ref[0], right_ref[1])
    s_real, s_imag = s[:, :root], s[:, root:]
    c = jnp.concatenate([s_real * h_real - s_imag * h_imag, s_real * h_imag + s_imag * h_real], axis=1)
    d = dot3(*split(c), left_ref[0], left_ref[1])
    d_real, d_imag = d[:, :root], d[:, root:]
    e = jnp.concatenate(
        [d_real * cos_twist - d_imag * sin_twist, d_imag * cos_twist + d_real * sin_twist], axis=0
    )
    return dot3(right_ref[0], right_ref[1], *split(e)) * (1.0 / (root * root))


def series_kernel(
    n_low,
    n_high,
    chunks,
    dm_ref,
    delay_ref,
    raw_ref,
    weight_ref,
    base_ref,
    left_ref,
    right_ref,
    twist_ref,
    out_ref,
    peak_ref,
    *scratch,
):
    got, partial, codes, landed, scale, scale_in = (scratch[2 * i : 2 * i + 2] for i in range(6))
    gather_send, gather_recv, sum_send, sum_recv, scale_send, scale_recv = (
        scratch[12 + 2 * i : 14 + 2 * i] for i in range(6)
    )
    chirp, flat, ready, ready_peak, middle, middle_peak = scratch[24:30]
    weight_refs, volt_ref, source, moved, signed = scratch[39:41], *scratch[41:]
    move_send, move_recv, peak_send, peak_recv, pass_send, pass_recv, last_send, last_recv, own_sem = scratch[30:39]
    n_sta, n_beams, n_sub, _, rows_out, _ = out_ref.shape
    root = twist_ref.shape[1]
    n_dev = n_sub * n_sta
    sub, sta = lax.axis_index("sub"), lax.axis_index("sta")
    sub_peer = lambda k: lax.rem(sub + k, n_sub)
    sta_peer = lambda k: lax.rem(sta + k, n_sta)
    half = root // 2
    pitch = partial[0].shape[1] // weight_refs[0].shape[0]
    blocks = volt_ref.shape[0] // 2 // chunks

    barrier = pltpu.get_barrier_semaphore()

    for k in range(1, n_sub):
        pl.semaphore_signal(barrier, inc=1, device_id=(sub_peer(k), sta), device_id_type=MESH)
    for k in range(1, n_sta):
        pl.semaphore_signal(barrier, inc=1, device_id=(sub, sta_peer(k)), device_id_type=MESH)
    pl.semaphore_wait(barrier, n_sub + n_sta - 2)

    stations, total_len = raw_ref.shape[1:]
    depth = 2 * stations
    spread_rows = depth + 4
    all_blocks = total_len // 128

    def unpack(i, carry):
        for u in range(8):
            block = i * 8 + u
            for part in range(2):
                source[pl.ds(block * spread_rows + part * stations, stations), :] = raw_ref[
                    part, :, pl.ds(pl.multiple_of(block * 128, 128), 128)
                ].astype(jnp.float32)
        return carry

    lax.fori_loop(0, all_blocks // 8, unpack, 0)
    for block in range(16):
        source[pl.ds((all_blocks + block) * spread_rows, depth), :] = source[
            pl.ds(block * spread_rows, depth), :
        ]
    lane = lax.broadcasted_iota(jnp.int32, (8, 128), 1)

    def gather(side, k, chunk):
        return pltpu.make_async_remote_copy(
            src_ref=volt_ref.at[pl.ds((side * chunks + chunk) * blocks, blocks)],
            dst_ref=got[side].at[k, pl.ds(chunk * blocks, blocks)],
            send_sem=gather_send[side].at[k, chunk],
            recv_sem=gather_recv[side].at[k, chunk],
            device_id=peers(side, n_low, n_high)[0][k],
            device_id_type=MESH,
        )

    def shift_chunk(chunk, carry):
        for side in range(2):
            first = (side * chunks + chunk) * blocks

            def shift_rows(i, carry):
                for u in range(4):
                    row = i * 4 + u
                    delay = delay_ref[row & (stations - 1)]
                    fine, coarse = delay & 127, delay >> 7
                    keep_lanes = lane < 128 - fine
                    for step in range(0, blocks, 8):
                        start = (first + step - coarse - 1) & (all_blocks - 1)
                        before = source[pl.ds(start * spread_rows + row, 8, stride=spread_rows), :]
                        after = source[pl.ds((start + 1) * spread_rows + row, 8, stride=spread_rows), :]
                        moved[pl.ds(step * spread_rows + row, 8, stride=spread_rows), :] = pltpu.roll(
                            jnp.where(keep_lanes, after, before), fine, 1
                        )
                return carry

            lax.fori_loop(0, depth // 4, shift_rows, 0)

            def pack(i, carry):
                for u in range(8):
                    block = i * 8 + u
                    volt_ref[first + block] = moved[pl.ds(block * spread_rows, depth), :].astype(volt_ref.dtype)
                return carry

            lax.fori_loop(0, blocks // 8, pack, 0)
            for k in range(len(peers(side, n_low, n_high)[0])):
                gather(side, k, chunk).start()
        return carry

    lax.fori_loop(0, chunks, shift_chunk, 0)

    high, low = sta // n_low, lax.rem(sta, n_low)
    for side, count in enumerate((n_low, n_high)):
        wanted = lax.broadcasted_iota(jnp.int32, (weight_ref.shape[2], count * depth), 0)
        column = lax.broadcasted_iota(jnp.int32, wanted.shape, 1)
        picks = []
        for part in range(2):
            station = jnp.full(wanted.shape, -1, jnp.int32)
            for k in range(count):
                in_row = high * n_low + lax.rem(low - k + n_low, n_low)
                in_column = lax.rem(high - k + n_high, n_high) * n_low + low
                owner = (in_row, in_column)[side]
                begin = k * depth + part * stations
                inside = (column >= begin) & (column < begin + stations)
                station = jnp.where(inside, column - begin + owner * stations, station)
            picks.append((wanted == station).astype(jnp.float32).astype(jnp.bfloat16))
        pick = lambda part, where: jnp.dot(weight_ref[part], picks[where], preferred_element_type=jnp.float32)
        signed[0, :, : count * depth] = pick(0, 0) - pick(1, 1)
        signed[1, :, : count * depth] = pick(1, 0) + pick(0, 1)
        for k in range((n_high, n_low)[side]):
            in_column = lax.rem(high + k, n_high) * n_low + low
            in_row = high * n_low + lax.rem(low + k, n_low)
            owner = (in_column, in_row)[side]
            for part in range(2):
                begin = (k * 2 + part) * n_beams
                weight_refs[side][begin : begin + n_beams, :] = signed[
                    part, pl.ds(owner * n_beams, n_beams), : count * depth
                ]

    def turns(beam, carry):
        measure = DM_STEP * dm_ref[beam].astype(jnp.float32)
        for part in range(0, root, 64):
            chirp[beam, 0, part : part + 64], chirp[beam, 1, part : part + 64] = turn(
                measure * base_ref[0, part : part + 64]
            )
        return carry

    lax.fori_loop(0, n_beams, turns, 0)

    for chunk in range(chunks):
        for side in range(2):
            members = len(peers(side, n_low, n_high)[0])
            for k in range(members):
                gather(side, k, chunk).wait_recv()
            weights = weight_refs[side][...].astype(jnp.bfloat16)

            def rows(i, carry):
                for u in range(8):
                    row = chunk * (blocks // 2) + i * 8 + u
                    own = side * (volt_ref.shape[0] // 2) + 2 * row
                    tall = [
                        jnp.concatenate([ref[at], ref[at + 1]], axis=1)
                        for ref, at in ((volt_ref, own), *((got[side].at[k], 2 * row) for k in range(members)))
                    ]
                    sums = jnp.dot(weights, jnp.concatenate(tall, axis=0), preferred_element_type=jnp.float32)
                    for lanes in range(2):
                        for base in range(0, weights.shape[0], 8):
                            partial[side][lanes, pl.ds(base * pitch + row, 8, stride=pitch), :] = sums[
                                base : base + 8, lanes * 128 : (lanes + 1) * 128
                            ]
                return carry

            lax.fori_loop(0, blocks // 16, rows, 0)

    def piece(side, k, part, beam, lanes):
        return partial[side][lanes, pl.ds(((k * 2 + part) * n_beams + beam) * pitch, half), :]

    for side in range(2):
        for k in range(len(peers(side, n_low, n_high)[1])):

            def encode(beam, carry):
                for lanes in range(2):
                    values = [piece(side, k + 1, part, beam, lanes) for part in range(2)]
                    ceiling = jnp.max(jnp.maximum(jnp.abs(values[0]), jnp.abs(values[1])), axis=0, keepdims=True)
                    scale[side][k, beam, lanes : lanes + 1, :] = ceiling
                    for part in range(2):
                        codes[side][k, beam, part, lanes] = quantize(values[part], ceiling)
                return carry

            lax.fori_loop(0, n_beams, encode, 0)

    scales = {}
    for side in range(2):
        for k, peer in enumerate(peers(side, n_low, n_high)[1]):
            scales[side, k] = pltpu.make_async_remote_copy(
                src_ref=scale[side].at[k],
                dst_ref=scale_in[side].at[k],
                send_sem=scale_send[side].at[k],
                recv_sem=scale_recv[side].at[k],
                device_id=peer,
                device_id_type=MESH,
            )
            scales[side, k].start()

    def exchange(side, k, beam):
        return pltpu.make_async_remote_copy(
            src_ref=codes[side].at[k, beam],
            dst_ref=landed[side].at[k, beam],
            send_sem=sum_send[side].at[k, beam],
            recv_sem=sum_recv[side].at[k, beam],
            device_id=peers(side, n_low, n_high)[1][k],
            device_id_type=MESH,
        )

    def each_exchange(beam, act):
        for side in range(2):
            for k in range(len(peers(side, n_low, n_high)[1])):
                act(exchange(side, k, beam))

    def launch(beam, carry):
        each_exchange(beam, lambda copy: copy.start())
        return carry

    lax.fori_loop(0, n_beams, launch, 0)
    for copy in scales.values():
        copy.wait_recv()

    def move(beam, k):
        return pltpu.make_async_remote_copy(
            src_ref=ready.at[sub_peer(k), beam],
            dst_ref=middle.at[beam, sub],
            send_sem=move_send.at[beam, k - 1],
            recv_sem=move_recv.at[beam, k - 1],
            device_id=(sub_peer(k), sta),
            device_id_type=MESH,
        )

    def move_peak(k):
        return pltpu.make_async_remote_copy(
            src_ref=ready_peak,
            dst_ref=middle_peak.at[sub],
            send_sem=peak_send.at[k - 1],
            recv_sem=peak_recv.at[k - 1],
            device_id=(sub_peer(k), sta),
            device_id_type=MESH,
        )

    def forward(beam, k):
        return pltpu.make_async_remote_copy(
            src_ref=middle.at[beam, :, sta_peer(k)],
            dst_ref=out_ref.at[sta, beam],
            send_sem=pass_send.at[beam, k - 1],
            recv_sem=pass_recv.at[beam, k - 1],
            device_id=(sub, sta_peer(k)),
            device_id_type=MESH,
        )

    def forward_peak(k):
        return pltpu.make_async_remote_copy(
            src_ref=middle_peak,
            dst_ref=peak_ref.at[sta],
            send_sem=last_send.at[k - 1],
            recv_sem=last_recv.at[k - 1],
            device_id=(sub, sta_peer(k)),
            device_id_type=MESH,
        )

    def keep(beam):
        return pltpu.make_async_copy(middle.at[beam, :, sta], out_ref.at[sta, beam], own_sem.at[beam])

    def finish(beam, carry):
        each_exchange(beam, lambda copy: copy.wait_recv())
        quarters = []
        for part in range(2):
            for side in range(2):
                pair = []
                for lanes in range(2):
                    total = piece(side, 0, part, beam, lanes)
                    for k in range(len(peers(side, n_low, n_high)[1])):
                        ceiling = scale_in[side][k, beam, lanes : lanes + 1, :]
                        total = total + dequantize(landed[side][k, beam, part, lanes], ceiling)
                    pair.append(total)
                quarters.append(jnp.concatenate(pair, axis=1))
        x = jnp.concatenate(quarters, axis=0)
        series = disperse(x, chirp[beam, 0], chirp[beam, 1], left_ref, right_ref, twist_ref)
        for part in range(2):
            for lanes in range(2):
                flat[part, pl.ds(lanes, root, 2), :] = series[
                    part * root : (part + 1) * root, lanes * half : (lanes + 1) * half
                ]
        values = [flat[part] for part in range(2)]
        ceiling = jnp.max(jnp.maximum(jnp.abs(values[0]), jnp.abs(values[1])), axis=0, keepdims=True)
        ready_peak[pl.ds(beam, 1), :] = ceiling
        for part in range(2):
            ready[:, beam, :, part] = quantize(values[part], ceiling).reshape(n_sub, n_sta, rows_out, half)
        middle[beam, sub] = ready[sub, beam]
        for k in range(1, n_sub):
            move(beam, k).start()
        return carry

    lax.fori_loop(0, n_beams, finish, 0)
    middle_peak[sub] = ready_peak[...]
    for k in range(1, n_sub):
        move_peak(k).start()

    def spread(beam, carry):
        for k in range(1, n_sub):
            move(beam, k).wait_recv()
        for k in range(1, n_sta):
            forward(beam, k).start()
        keep(beam).start()
        return carry

    lax.fori_loop(0, n_beams, spread, 0)
    for k in range(1, n_sub):
        move_peak(k).wait_recv()
    for k in range(1, n_sta):
        forward_peak(k).start()
    own_peak = pltpu.make_async_copy(middle_peak, peak_ref.at[sta], own_sem.at[n_beams])
    own_peak.start()

    def drain(beam, carry):
        each_exchange(beam, lambda copy: copy.wait_send())
        return carry

    lax.fori_loop(0, n_beams, drain, 0)
    for copy in scales.values():
        copy.wait_send()
    for chunk in range(chunks):
        for side in range(2):
            for k in range(len(peers(side, n_low, n_high)[0])):
                gather(side, k, chunk).wait_send()
    own_peak.wait()
    for k in range(1, n_sub):
        move_peak(k).wait_send()
    for k in range(1, n_sta):
        forward_peak(k).wait()

    def settle(beam, carry):
        keep(beam).wait()
        for k in range(1, n_sub):
            move(beam, k).wait_send()
        for k in range(1, n_sta):
            forward(beam, k).wait()
        return carry

    lax.fori_loop(0, n_beams, settle, 0)


def make_series(dm_index, delays, volts, weights, base_phase, n_low, n_high, n_sub, root):
    depth, blocks = 2 * volts.shape[1], volts.shape[2] // 128
    spread_rows = depth + 4
    chunks = 4
    n_beams = dm_index.shape[0]
    half = root // 2
    n_sta = n_low * n_high
    rows_out = 2 * root // (n_sub * n_sta)
    tables = dft_tables(root)
    vmem = pl.BlockSpec(memory_space=pltpu.VMEM)
    hbm = pl.BlockSpec(memory_space=pltpu.HBM)
    pitch = half + 4
    dma = pltpu.SemaphoreType.DMA
    groups = ((n_low, n_high), (n_high, n_low))
    per_side = lambda make: [make(*group) for group in groups]
    return pl.pallas_call(
        functools.partial(series_kernel, n_low, n_high, chunks),
        in_specs=[*[pl.BlockSpec(memory_space=pltpu.SMEM)] * 2, *[vmem] * 6],
        out_specs=(hbm, hbm),
        out_shape=(
            jax.ShapeDtypeStruct((n_sta, n_beams, n_sub, 2, rows_out, 128), jnp.int16),
            jax.ShapeDtypeStruct((n_sta, n_sub, n_beams, 128), jnp.float32),
        ),
        scratch_shapes=[
            *per_side(lambda g, r: pltpu.VMEM((g - 1, blocks // 2, depth, 128), jnp.bfloat16)),
            *per_side(lambda g, r: pltpu.VMEM((2, r * 2 * n_beams * pitch, 128), jnp.float32)),
            *per_side(lambda g, r: pltpu.VMEM((r - 1, n_beams, 2, 2, half, 128), jnp.int16)),
            *per_side(lambda g, r: pltpu.VMEM((r - 1, n_beams, 2, 2, half, 128), jnp.int16)),
            *per_side(lambda g, r: pltpu.VMEM((r - 1, n_beams, 8, 128), jnp.float32)),
            *per_side(lambda g, r: pltpu.VMEM((r - 1, n_beams, 8, 128), jnp.float32)),
            *per_side(lambda g, r: dma((g - 1, chunks))),
            *per_side(lambda g, r: dma((g - 1, chunks))),
            *per_side(lambda g, r: dma((r - 1, n_beams))),
            *per_side(lambda g, r: dma((r - 1, n_beams))),
            *per_side(lambda g, r: dma((r - 1,))),
            *per_side(lambda g, r: dma((r - 1,))),
            pltpu.VMEM((n_beams, 2, root, root), jnp.float32),
            pltpu.VMEM((2, 2 * root, 128), jnp.float32),
            pltpu.VMEM((n_sub, n_beams, n_sta, 2, rows_out, 128), jnp.int16),
            pltpu.VMEM((n_beams, 128), jnp.float32),
            pltpu.VMEM((n_beams, n_sub, n_sta, 2, rows_out, 128), jnp.int16),
            pltpu.VMEM((n_sub, n_beams, 128), jnp.float32),
            dma((n_beams, n_sub - 1)),
            dma((n_beams, n_sub - 1)),
            dma((n_sub - 1,)),
            dma((n_sub - 1,)),
            dma((n_beams, n_sta - 1)),
            dma((n_beams, n_sta - 1)),
            dma((n_sta - 1,)),
            dma((n_sta - 1,)),
            dma((n_beams + 1,)),
            *per_side(lambda g, r: pltpu.VMEM((r * 2 * n_beams, g * depth), jnp.float32)),
            pltpu.VMEM((blocks, depth, 128), jnp.bfloat16),
            pltpu.VMEM(((blocks + 16) * spread_rows, 128), jnp.float32),
            pltpu.VMEM((blocks // 2 // chunks * spread_rows, 128), jnp.float32),
            pltpu.VMEM((2, weights.shape[1], 128), jnp.float32),
        ],
        compiler_params=pltpu.CompilerParams(
            collective_id=0, has_side_effects=True, vmem_limit_bytes=60 * 1024 * 1024
        ),
        cost_estimate=pl.CostEstimate(
            flops=8 * n_beams * depth * blocks * 128, bytes_accessed=2 * volts.size, transcendentals=0
        ),
    )(dm_index[:, 0], delays, volts, weights, base_phase, *tables)


def shards(voltages, beam_weights, station_delays, dm_index):
    sub_dev = voltages.shape[0]
    total_len = voltages.shape[3]
    local_beams = dm_index.shape[0]
    trials = dm_index.shape[1]
    root_len = int(round(total_len**0.5))
    n_sub = lax.axis_size("sub")
    n_sta = lax.axis_size("sta")
    assert sub_dev == 1 and trials == 1 and root_len * root_len == total_len
    n_low = 2 if n_sta % 2 == 0 else 1
    n_high = n_sta // n_low
    subband = lax.axis_index("sub") + jnp.arange(1, dtype=jnp.int32)
    base_phase = chirp_base(subband, root_len, total_len)
    codes, peak = make_series(
        dm_index, station_delays, voltages[0], beam_weights[0], base_phase, n_low, n_high, n_sub, root_len
    )
    peak = peak.transpose(1, 0, 2, 3)[:, None, :, :, None, :]
    moved = dequantize(codes.transpose(2, 3, 0, 1, 4, 5), peak)
    moved = moved.reshape(n_sub, 2, n_sta * local_beams, *moved.shape[4:])
    intensity = jnp.mean(moved[:, 0] * moved[:, 0] + moved[:, 1] * moved[:, 1], axis=0)
    return (moved.reshape(*moved.shape[:3], 1, -1), intensity.reshape(intensity.shape[0], 1, -1))


def solution(mesh):
    return jax.shard_map(
        shards,
        mesh=mesh,
        in_specs=(
            P("sub", None, "sta", None),
            P("sub", None, None, None),
            P("sta"),
            P("sta", None),
        ),
        out_specs=(P(None, None, None, None, ("sub", "sta")), P(None, None, ("sub", "sta"))),
        check_vma=False,
    )
```

```python
import functools

import jax
import jax.numpy as jnp
import numpy as np
from jax import lax
from jax.experimental import pallas as pl
from jax.experimental.pallas import tpu as pltpu
from jax.sharding import PartitionSpec as P


TWO_PI = 6.283185307179586
DISPERSION = 4148808000.0
DM_STEP = 10.0
BASE_FREQ = 120.0
CHANNEL_WIDTH = 0.1953125


def dft_tables(root_len):
    total_len = root_len * root_len
    product = np.outer(np.arange(root_len), np.arange(root_len))
    root_angle = 2 * np.pi * (product % root_len) / root_len
    cos_root, sin_root = np.cos(root_angle), np.sin(root_angle)
    left = np.block([[cos_root, sin_root], [-sin_root, cos_root]]).astype(np.float32)
    high = left.astype(jnp.bfloat16)
    low = (left - high.astype(np.float32)).astype(jnp.bfloat16)
    twist_angle = 2 * np.pi * product / total_len
    twist = np.stack([np.cos(twist_angle), np.sin(twist_angle)]).astype(np.float32)
    return np.stack([high, low]), np.stack([high.T, low.T]), twist


def chirp_base(subband, root_len, total_len):
    first = jnp.arange(root_len, dtype=jnp.int32)[:, None]
    second = jnp.arange(root_len, dtype=jnp.int32)[None, :]
    positions = first + root_len * second
    signed_bin = jnp.where(positions < total_len // 2, positions, positions - total_len)
    offset = (CHANNEL_WIDTH * signed_bin.astype(jnp.float32) / total_len)[None]
    centre = (BASE_FREQ + CHANNEL_WIDTH * (subband.astype(jnp.float32) + 0.5))[:, None, None]
    return TWO_PI * DISPERSION * offset * offset / (centre * centre * (centre + offset))


def split(values):
    high = values.astype(jnp.bfloat16)
    return high, (values - high.astype(jnp.float32)).astype(jnp.bfloat16)


def dot3(a_high, a_low, b_high, b_low):
    dot = functools.partial(jnp.dot, preferred_element_type=jnp.float32)
    return dot(a_high, b_high) + (dot(a_high, b_low) + dot(a_low, b_high))


MESH = pl.DeviceIdType.MESH
PEAK = 32767.0


def peers(side, n_low, n_high):
    sub, sta = lax.axis_index("sub"), lax.axis_index("sta")
    high, low = sta // n_low, lax.rem(sta, n_low)
    along = (
        [(sub, high * n_low + lax.rem(low + k, n_low)) for k in range(1, n_low)],
        [(sub, lax.rem(high + k, n_high) * n_low + low) for k in range(1, n_high)],
    )
    return along[side], along[1 - side]


def quantize(values, ceiling):
    return jnp.round(values * (PEAK / jnp.maximum(ceiling, 1e-30))).astype(jnp.int32).astype(jnp.int16)


def dequantize(codes, ceiling):
    return codes.astype(jnp.int32).astype(jnp.float32) * (ceiling * (1.0 / PEAK))


def turn(phase):
    count = jnp.round(phase * 0.6366197723675814)
    rest = ((phase - count * 1.5703125) - count * 4.837512969970703125e-4) - count * 7.54978995489188216e-8
    square = rest * rest
    sine = rest + rest * square * (
        (-1.9515295891e-4 * square + 8.3321608736e-3) * square - 1.6666654611e-1
    )
    cosine = (1.0 - 0.5 * square) + square * square * (
        (2.443315711809948e-5 * square - 1.388731625493765e-3) * square + 4.166664568298827e-2
    )
    quarter = count.astype(jnp.int32)
    odd = (quarter & 1) == 1
    real, imag = jnp.where(odd, sine, cosine), jnp.where(odd, cosine, sine)
    real = jnp.where(((quarter + 1) & 2) == 2, -real, real)
    imag = jnp.where((quarter & 2) == 2, -imag, imag)
    return real, imag


def disperse(x, h_real, h_imag, left_ref, right_ref, twist_ref):
    root = twist_ref.shape[1]
    cos_twist, sin_twist = twist_ref[0], twist_ref[1]
    a = dot3(left_ref[0], left_ref[1], *split(x))
    a_real, a_imag = a[:root], a[root:]
    b = jnp.concatenate(
        [a_real * cos_twist + a_imag * sin_twist, a_imag * cos_twist - a_real * sin_twist], axis=1
    )
    s = dot3(*split(b), right_ref[0], right_ref[1])
    s_real, s_imag = s[:, :root], s[:, root:]
    c = jnp.concatenate([s_real * h_real - s_imag * h_imag, s_real * h_imag + s_imag * h_real], axis=1)
    d = dot3(*split(c), left_ref[0], left_ref[1])
    d_real, d_imag = d[:, :root], d[:, root:]
    e = jnp.concatenate(
        [d_real * cos_twist - d_imag * sin_twist, d_imag * cos_twist + d_real * sin_twist], axis=0
    )
    return dot3(right_ref[0], right_ref[1], *split(e)) * (1.0 / (root * root))


def series_kernel(
    n_low,
    n_high,
    chunks,
    dm_ref,
    delay_ref,
    raw_ref,
    weight_ref,
    base_ref,
    left_hbm,
    right_hbm,
    twist_hbm,
    out_ref,
    peak_ref,
    *scratch,
):
    got, partial, codes, landed, scale, scale_in = (scratch[2 * i : 2 * i + 2] for i in range(6))
    gather_send, gather_recv, sum_send, sum_recv, scale_send, scale_recv = (
        scratch[12 + 2 * i : 14 + 2 * i] for i in range(6)
    )
    chirp, flat, ready, ready_peak, middle, middle_peak = scratch[24:30]
    weight_refs, volt_ref, source, moved, signed = scratch[39:41], *scratch[41:45]
    left_ref, right_ref, twist_ref, table_sem = scratch[45:]
    tables = [
        pltpu.make_async_copy(left_hbm, left_ref, table_sem.at[0]),
        pltpu.make_async_copy(right_hbm, right_ref, table_sem.at[1]),
        pltpu.make_async_copy(twist_hbm, twist_ref, table_sem.at[2]),
    ]
    move_send, move_recv, peak_send, peak_recv, pass_send, pass_recv, last_send, last_recv, own_sem = scratch[30:39]
    n_sta, n_beams, n_sub, _, rows_out, _ = out_ref.shape
    root = twist_hbm.shape[1]
    n_dev = n_sub * n_sta
    sub, sta = lax.axis_index("sub"), lax.axis_index("sta")
    sub_peer = lambda k: lax.rem(sub + k, n_sub)
    sta_peer = lambda k: lax.rem(sta + k, n_sta)
    half = root // 2
    pitch = partial[0].shape[1] // weight_refs[0].shape[0]
    blocks = volt_ref.shape[0] // 2 // chunks

    barrier = pltpu.get_barrier_semaphore()

    for k in range(1, n_sub):
        pl.semaphore_signal(barrier, inc=1, device_id=(sub_peer(k), sta), device_id_type=MESH)
    for k in range(1, n_sta):
        pl.semaphore_signal(barrier, inc=1, device_id=(sub, sta_peer(k)), device_id_type=MESH)
    for copy in tables:
        copy.start()

    stations, total_len = raw_ref.shape[1:]
    depth = 2 * stations
    spread_rows = depth + 4
    all_blocks = total_len // 128

    def unpack(i, carry):
        for u in range(8):
            block = i * 8 + u
            for part in range(2):
                source[pl.ds(block * spread_rows + part * stations, stations), :] = raw_ref[
                    part, :, pl.ds(pl.multiple_of(block * 128, 128), 128)
                ].astype(jnp.float32)
        return carry

    lax.fori_loop(0, all_blocks // 8, unpack, 0)
    for block in range(16):
        source[pl.ds((all_blocks + block) * spread_rows, depth), :] = source[
            pl.ds(block * spread_rows, depth), :
        ]
    lane = lax.broadcasted_iota(jnp.int32, (8, 128), 1)
    pl.semaphore_wait(barrier, n_sub + n_sta - 2)

    def gather(side, k, chunk):
        return pltpu.make_async_remote_copy(
            src_ref=volt_ref.at[pl.ds((side * chunks + chunk) * blocks, blocks)],
            dst_ref=got[side].at[k, pl.ds(chunk * blocks, blocks)],
            send_sem=gather_send[side].at[k],
            recv_sem=gather_recv[side].at[k, chunk],
            device_id=peers(side, n_low, n_high)[0][k],
            device_id_type=MESH,
        )

    def shift_chunk(chunk, carry):
        for side in range(2):
            first = (side * chunks + chunk) * blocks

            def shift_rows(i, carry):
                for u in range(4):
                    row = i * 4 + u
                    delay = delay_ref[row & (stations - 1)]
                    fine, coarse = delay & 127, delay >> 7
                    keep_lanes = lane < 128 - fine
                    for step in range(0, blocks, 8):
                        start = (first + step - coarse - 1) & (all_blocks - 1)
                        before = source[pl.ds(start * spread_rows + row, 8, stride=spread_rows), :]
                        after = source[pl.ds((start + 1) * spread_rows + row, 8, stride=spread_rows), :]
                        moved[pl.ds(step * spread_rows + row, 8, stride=spread_rows), :] = pltpu.roll(
                            jnp.where(keep_lanes, after, before), fine, 1
                        )
                return carry

            lax.fori_loop(0, depth // 4, shift_rows, 0)

            def pack(i, carry):
                for u in range(8):
                    block = i * 8 + u
                    volt_ref[first + block] = moved[pl.ds(block * spread_rows, depth), :].astype(volt_ref.dtype)
                return carry

            lax.fori_loop(0, blocks // 8, pack, 0)
            for k in range(len(peers(side, n_low, n_high)[0])):
                gather(side, k, chunk).start()
        return carry

    lax.fori_loop(0, chunks, shift_chunk, 0)

    high, low = sta // n_low, lax.rem(sta, n_low)
    for side, count in enumerate((n_low, n_high)):
        wanted = lax.broadcasted_iota(jnp.int32, (weight_ref.shape[2], count * depth), 0)
        column = lax.broadcasted_iota(jnp.int32, wanted.shape, 1)
        picks = []
        for part in range(2):
            station = jnp.full(wanted.shape, -1, jnp.int32)
            for k in range(count):
                in_row = high * n_low + lax.rem(low - k + n_low, n_low)
                in_column = lax.rem(high - k + n_high, n_high) * n_low + low
                owner = (in_row, in_column)[side]
                begin = k * depth + part * stations
                inside = (column >= begin) & (column < begin + stations)
                station = jnp.where(inside, column - begin + owner * stations, station)
            picks.append((wanted == station).astype(jnp.float32).astype(jnp.bfloat16))
        pick = lambda part, where: jnp.dot(weight_ref[part], picks[where], preferred_element_type=jnp.float32)
        signed[0, :, : count * depth] = pick(0, 0) - pick(1, 1)
        signed[1, :, : count * depth] = pick(1, 0) + pick(0, 1)
        for k in range((n_high, n_low)[side]):
            in_column = lax.rem(high + k, n_high) * n_low + low
            in_row = high * n_low + lax.rem(low + k, n_low)
            owner = (in_column, in_row)[side]
            for part in range(2):
                begin = (k * 2 + part) * n_beams
                weight_refs[side][begin : begin + n_beams, :] = signed[
                    part, pl.ds(owner * n_beams, n_beams), : count * depth
                ]

    def turns(beam, carry):
        measure = DM_STEP * dm_ref[beam].astype(jnp.float32)
        for part in range(0, root, 64):
            chirp[beam, 0, part : part + 64], chirp[beam, 1, part : part + 64] = turn(
                measure * base_ref[0, part : part + 64]
            )
        return carry

    lax.fori_loop(0, n_beams, turns, 0)

    for chunk in range(chunks):
        for side in range(2):
            members = len(peers(side, n_low, n_high)[0])
            for k in range(members):
                gather(side, k, chunk).wait_recv()
            weights = weight_refs[side][...].astype(jnp.bfloat16)

            def rows(i, carry):
                for u in range(8):
                    row = chunk * (blocks // 2) + i * 8 + u
                    own = side * (volt_ref.shape[0] // 2) + 2 * row
                    tall = [
                        jnp.concatenate([ref[at], ref[at + 1]], axis=1)
                        for ref, at in ((volt_ref, own), *((got[side].at[k], 2 * row) for k in range(members)))
                    ]
                    sums = jnp.dot(weights, jnp.concatenate(tall, axis=0), preferred_element_type=jnp.float32)
                    for lanes in range(2):
                        for base in range(0, weights.shape[0], 8):
                            partial[side][lanes, pl.ds(base * pitch + row, 8, stride=pitch), :] = sums[
                                base : base + 8, lanes * 128 : (lanes + 1) * 128
                            ]
                return carry

            lax.fori_loop(0, blocks // 16, rows, 0)

    def piece(side, k, part, beam, lanes):
        return partial[side][lanes, pl.ds(((k * 2 + part) * n_beams + beam) * pitch, half), :]

    def exchange(side, k, beam):
        return pltpu.make_async_remote_copy(
            src_ref=codes[side].at[k, beam],
            dst_ref=landed[side].at[k, beam],
            send_sem=sum_send[side].at[k],
            recv_sem=sum_recv[side].at[k, beam],
            device_id=peers(side, n_low, n_high)[1][k],
            device_id_type=MESH,
        )

    def exchange_scale(side, k, beam):
        return pltpu.make_async_remote_copy(
            src_ref=scale[side].at[k, beam],
            dst_ref=scale_in[side].at[k, beam],
            send_sem=scale_send[side].at[k],
            recv_sem=scale_recv[side].at[k, beam],
            device_id=peers(side, n_low, n_high)[1][k],
            device_id_type=MESH,
        )

    def encode(beam, carry):
        for side in range(2):
            for k in range(len(peers(side, n_low, n_high)[1])):
                for lanes in range(2):
                    values = [piece(side, k + 1, part, beam, lanes) for part in range(2)]
                    ceiling = jnp.max(jnp.maximum(jnp.abs(values[0]), jnp.abs(values[1])), axis=0, keepdims=True)
                    scale[side][k, beam, lanes : lanes + 1, :] = ceiling
                    for part in range(2):
                        codes[side][k, beam, part, lanes] = quantize(values[part], ceiling)
                exchange_scale(side, k, beam).start()
                exchange(side, k, beam).start()
        return carry

    lax.fori_loop(0, n_beams, encode, 0)
    for copy in tables:
        copy.wait()

    def total_of(ref, send_sem, recv_sem):
        return pltpu.make_async_remote_copy(
            src_ref=ref, dst_ref=ref, send_sem=send_sem, recv_sem=recv_sem, device_id=(sub, sta), device_id_type=MESH
        )

    def move(beam, k):
        return pltpu.make_async_remote_copy(
            src_ref=ready.at[sub_peer(k), beam],
            dst_ref=middle.at[beam, sub],
            send_sem=move_send.at[k - 1],
            recv_sem=move_recv.at[beam],
            device_id=(sub_peer(k), sta),
            device_id_type=MESH,
        )

    def move_peak(k):
        return pltpu.make_async_remote_copy(
            src_ref=ready_peak,
            dst_ref=middle_peak.at[sub],
            send_sem=peak_send,
            recv_sem=peak_recv,
            device_id=(sub_peer(k), sta),
            device_id_type=MESH,
        )

    def forward(beam, k):
        return pltpu.make_async_remote_copy(
            src_ref=middle.at[beam, :, sta_peer(k)],
            dst_ref=out_ref.at[sta, beam],
            send_sem=pass_send.at[k - 1],
            recv_sem=pass_recv.at[k - 1],
            device_id=(sub, sta_peer(k)),
            device_id_type=MESH,
        )

    def forward_peak(k):
        return pltpu.make_async_remote_copy(
            src_ref=middle_peak,
            dst_ref=peak_ref.at[sta],
            send_sem=last_send,
            recv_sem=last_recv,
            device_id=(sub, sta_peer(k)),
            device_id_type=MESH,
        )

    def keep(beam):
        return pltpu.make_async_copy(middle.at[beam, :, sta], out_ref.at[sta, beam], own_sem.at[0])

    def finish(beam, carry):
        for side in range(2):
            for k in range(len(peers(side, n_low, n_high)[1])):
                exchange_scale(side, k, beam).wait_recv()
                exchange(side, k, beam).wait_recv()
        quarters = []
        for part in range(2):
            for side in range(2):
                pair = []
                for lanes in range(2):
                    total = piece(side, 0, part, beam, lanes)
                    for k in range(len(peers(side, n_low, n_high)[1])):
                        ceiling = scale_in[side][k, beam, lanes : lanes + 1, :]
                        total = total + dequantize(landed[side][k, beam, part, lanes], ceiling)
                    pair.append(total)
                quarters.append(jnp.concatenate(pair, axis=1))
        x = jnp.concatenate(quarters, axis=0)
        series = disperse(x, chirp[beam, 0], chirp[beam, 1], left_ref, right_ref, twist_ref)
        for part in range(2):
            for lanes in range(2):
                flat[part, pl.ds(lanes, root, 2), :] = series[
                    part * root : (part + 1) * root, lanes * half : (lanes + 1) * half
                ]
        values = [flat[part] for part in range(2)]
        ceiling = jnp.max(jnp.maximum(jnp.abs(values[0]), jnp.abs(values[1])), axis=0, keepdims=True)
        ready_peak[pl.ds(beam, 1), :] = ceiling
        for part in range(2):
            ready[:, beam, :, part] = quantize(values[part], ceiling).reshape(n_sub, n_sta, rows_out, half)
        middle[beam, sub] = ready[sub, beam]
        for k in range(1, n_sub):
            move(beam, k).start()
        return carry

    lax.fori_loop(0, n_beams, finish, 0)
    middle_peak[sub] = ready_peak[...]
    for k in range(1, n_sub):
        move_peak(k).start()

    def spread(beam, carry):
        total_of(middle.at[beam, pl.ds(0, n_sub - 1)], move_send.at[0], move_recv.at[beam]).wait_recv()
        for k in range(1, n_sta):
            forward(beam, k).start()
        keep(beam).start()
        return carry

    lax.fori_loop(0, n_beams, spread, 0)
    arrived = middle_peak.at[pl.ds(0, n_sub - 1)]
    total_of(arrived, peak_send, peak_recv).wait_recv()
    for k in range(1, n_sta):
        forward_peak(k).start()
    own_peak = pltpu.make_async_copy(middle_peak, peak_ref.at[sta], own_sem.at[1])
    own_peak.start()

    for side in range(2):
        whole = volt_ref.at[pl.ds(side * chunks * blocks, chunks * blocks)]
        for k in range(len(peers(side, n_low, n_high)[0])):
            total_of(whole, gather_send[side].at[k], gather_send[side].at[k]).wait_send()
        for k in range(len(peers(side, n_low, n_high)[1])):
            total_of(codes[side].at[k], sum_send[side].at[k], sum_send[side].at[k]).wait_send()
            total_of(scale[side].at[k], scale_send[side].at[k], scale_send[side].at[k]).wait_send()
    for k in range(1, n_sub):
        total_of(ready.at[sub_peer(k)], move_send.at[k - 1], move_send.at[k - 1]).wait_send()
    total_of(arrived, peak_send, peak_recv).wait_send()
    pltpu.make_async_copy(middle.at[:, :, sta], out_ref.at[sta], own_sem.at[0]).wait()
    own_peak.wait()
    for k in range(1, n_sta):
        total_of(middle.at[:, :, sta_peer(k)], pass_send.at[k - 1], pass_recv.at[k - 1]).wait_send()
        total_of(out_ref.at[sta_peer(k)], pass_send.at[k - 1], pass_recv.at[k - 1]).wait_recv()
    others = peak_ref.at[pl.ds(0, n_sta - 1)]
    total_of(others, last_send, last_recv).wait()


def make_series(dm_index, delays, volts, weights, base_phase, n_low, n_high, n_sub, root):
    depth, blocks = 2 * volts.shape[1], volts.shape[2] // 128
    spread_rows = depth + 4
    chunks = 8
    n_beams = dm_index.shape[0]
    half = root // 2
    n_sta = n_low * n_high
    rows_out = 2 * root // (n_sub * n_sta)
    tables = dft_tables(root)
    vmem = pl.BlockSpec(memory_space=pltpu.VMEM)
    hbm = pl.BlockSpec(memory_space=pltpu.HBM)
    pitch = half + 4
    dma = pltpu.SemaphoreType.DMA
    groups = ((n_low, n_high), (n_high, n_low))
    per_side = lambda make: [make(*group) for group in groups]
    return pl.pallas_call(
        functools.partial(series_kernel, n_low, n_high, chunks),
        in_specs=[*[pl.BlockSpec(memory_space=pltpu.SMEM)] * 2, *[vmem] * 3, *[hbm] * 3],
        out_specs=(hbm, hbm),
        out_shape=(
            jax.ShapeDtypeStruct((n_sta, n_beams, n_sub, 2, rows_out, 128), jnp.int16),
            jax.ShapeDtypeStruct((n_sta, n_sub, n_beams, 128), jnp.float32),
        ),
        scratch_shapes=[
            *per_side(lambda g, r: pltpu.VMEM((g - 1, blocks // 2, depth, 128), jnp.bfloat16)),
            *per_side(lambda g, r: pltpu.VMEM((2, r * 2 * n_beams * pitch, 128), jnp.float32)),
            *per_side(lambda g, r: pltpu.VMEM((r - 1, n_beams, 2, 2, half, 128), jnp.int16)),
            *per_side(lambda g, r: pltpu.VMEM((r - 1, n_beams, 2, 2, half, 128), jnp.int16)),
            *per_side(lambda g, r: pltpu.VMEM((r - 1, n_beams, 8, 128), jnp.float32)),
            *per_side(lambda g, r: pltpu.VMEM((r - 1, n_beams, 8, 128), jnp.float32)),
            *per_side(lambda g, r: dma((g - 1,))),
            *per_side(lambda g, r: dma((g - 1, chunks))),
            *per_side(lambda g, r: dma((r - 1,))),
            *per_side(lambda g, r: dma((r - 1, n_beams))),
            *per_side(lambda g, r: dma((r - 1,))),
            *per_side(lambda g, r: dma((r - 1, n_beams))),
            pltpu.VMEM((n_beams, 2, root, root), jnp.float32),
            pltpu.VMEM((2, 2 * root, 128), jnp.float32),
            pltpu.VMEM((n_sub, n_beams, n_sta, 2, rows_out, 128), jnp.int16),
            pltpu.VMEM((n_beams, 128), jnp.float32),
            pltpu.VMEM((n_beams, n_sub, n_sta, 2, rows_out, 128), jnp.int16),
            pltpu.VMEM((n_sub, n_beams, 128), jnp.float32),
            dma((n_sub - 1,)),
            dma((n_beams,)),
            dma,
            dma,
            dma((n_sta - 1,)),
            dma((n_sta - 1,)),
            dma,
            dma,
            dma((2,)),
            *per_side(lambda g, r: pltpu.VMEM((r * 2 * n_beams, g * depth), jnp.float32)),
            pltpu.VMEM((blocks, depth, 128), jnp.bfloat16),
            pltpu.VMEM(((blocks + 16) * spread_rows, 128), jnp.float32),
            pltpu.VMEM((blocks // 2 // chunks * spread_rows, 128), jnp.float32),
            pltpu.VMEM((2, weights.shape[1], 128), jnp.float32),
            *[pltpu.VMEM(table.shape, table.dtype) for table in tables],
            dma((3,)),
        ],
        compiler_params=pltpu.CompilerParams(
            collective_id=0, has_side_effects=True, vmem_limit_bytes=60 * 1024 * 1024
        ),
        cost_estimate=pl.CostEstimate(
            flops=8 * n_beams * depth * blocks * 128, bytes_accessed=2 * volts.size, transcendentals=0
        ),
    )(dm_index[:, 0], delays, volts, weights, base_phase, *tables)


def unpack_kernel(codes_ref, peak_ref, out_ref, power_ref):
    n_sub, _, n_beams = out_ref.shape[:3]
    for beam in range(n_beams):
        power = jnp.zeros(power_ref.shape[1:], jnp.float32)
        for sub in range(n_sub):
            for part in range(2):
                values = dequantize(codes_ref[0, beam, sub, part], peak_ref[0, sub, beam : beam + 1, :])
                out_ref[sub, part, beam] = values
                power = power + values * values
        power_ref[beam] = power * (1.0 / n_sub)


def unpack_series(codes, peak):
    n_sta, n_beams, n_sub, _, rows, lanes = codes.shape
    return pl.pallas_call(
        unpack_kernel,
        grid=(n_sta,),
        in_specs=[
            pl.BlockSpec((1, n_beams, n_sub, 2, rows, lanes), lambda i: (i, 0, 0, 0, 0, 0)),
            pl.BlockSpec((1, n_sub, n_beams, lanes), lambda i: (i, 0, 0, 0)),
        ],
        out_specs=[
            pl.BlockSpec((n_sub, 2, n_beams, rows, lanes), lambda i: (0, 0, i, 0, 0)),
            pl.BlockSpec((n_beams, rows, lanes), lambda i: (i, 0, 0)),
        ],
        out_shape=[
            jax.ShapeDtypeStruct((n_sub, 2, n_sta * n_beams, rows, lanes), jnp.float32),
            jax.ShapeDtypeStruct((n_sta * n_beams, rows, lanes), jnp.float32),
        ],
    )(codes, peak)


def shards(voltages, beam_weights, station_delays, dm_index):
    sub_dev = voltages.shape[0]
    total_len = voltages.shape[3]
    local_beams = dm_index.shape[0]
    trials = dm_index.shape[1]
    root_len = int(round(total_len**0.5))
    n_sub = lax.axis_size("sub")
    n_sta = lax.axis_size("sta")
    assert sub_dev == 1 and trials == 1 and root_len * root_len == total_len
    n_low = 2 if n_sta % 2 == 0 else 1
    n_high = n_sta // n_low
    subband = lax.axis_index("sub") + jnp.arange(1, dtype=jnp.int32)
    base_phase = chirp_base(subband, root_len, total_len)
    codes, peak = make_series(
        dm_index, station_delays, voltages[0], beam_weights[0], base_phase, n_low, n_high, n_sub, root_len
    )
    moved, intensity = unpack_series(codes, peak)
    return (moved.reshape(*moved.shape[:3], 1, -1), intensity.reshape(intensity.shape[0], 1, -1))


def solution(mesh):
    return jax.shard_map(
        shards,
        mesh=mesh,
        in_specs=(
            P("sub", None, "sta", None),
            P("sub", None, None, None),
            P("sta"),
            P("sta", None),
        ),
        out_specs=(P(None, None, None, None, ("sub", "sta")), P(None, None, ("sub", "sta"))),
        check_vma=False,
    )
```

```python
import functools

import jax
import jax.numpy as jnp
import numpy as np
from jax import lax
from jax.experimental import pallas as pl
from jax.experimental.pallas import tpu as pltpu
from jax.sharding import PartitionSpec as P


TWO_PI = 6.283185307179586
DISPERSION = 4148808000.0
DM_STEP = 10.0
BASE_FREQ = 120.0
CHANNEL_WIDTH = 0.1953125


def dft_tables(root_len):
    total_len = root_len * root_len
    product = np.outer(np.arange(root_len), np.arange(root_len))
    root_angle = 2 * np.pi * (product % root_len) / root_len
    cos_root, sin_root = np.cos(root_angle), np.sin(root_angle)
    left = np.block([[cos_root, sin_root], [-sin_root, cos_root]]).astype(np.float32)
    high = left.astype(jnp.bfloat16)
    low = (left - high.astype(np.float32)).astype(jnp.bfloat16)
    twist_angle = 2 * np.pi * product / total_len
    twist = np.stack([np.cos(twist_angle), np.sin(twist_angle)]).astype(np.float32)
    return np.stack([high, low]), np.stack([high.T, low.T]), twist


def chirp_base(subband, begin, rows, root_len):
    total_len = root_len * root_len
    first = lax.broadcasted_iota(jnp.int32, (rows, root_len), 0) + begin
    second = lax.broadcasted_iota(jnp.int32, (rows, root_len), 1)
    positions = first + root_len * second
    signed_bin = jnp.where(positions < total_len // 2, positions, positions - total_len)
    offset = CHANNEL_WIDTH * signed_bin.astype(jnp.float32) / total_len
    band = jnp.full((rows, root_len), subband, jnp.int32).astype(jnp.float32)
    centre = BASE_FREQ + CHANNEL_WIDTH * (band + 0.5)
    return TWO_PI * DISPERSION * offset * offset / (centre * centre * (centre + offset))


def split(values):
    high = values.astype(jnp.bfloat16)
    return high, (values - high.astype(jnp.float32)).astype(jnp.bfloat16)


def dot3(a_high, a_low, b_high, b_low):
    dot = functools.partial(jnp.dot, preferred_element_type=jnp.float32)
    return dot(a_high, b_high) + (dot(a_high, b_low) + dot(a_low, b_high))


MESH = pl.DeviceIdType.MESH
PEAK = 32767.0


def peers(side, n_low, n_high):
    sub, sta = lax.axis_index("sub"), lax.axis_index("sta")
    high, low = sta // n_low, lax.rem(sta, n_low)
    along = (
        [(sub, high * n_low + lax.rem(low + k, n_low)) for k in range(1, n_low)],
        [(sub, lax.rem(high + k, n_high) * n_low + low) for k in range(1, n_high)],
    )
    return along[side], along[1 - side]


def quantize(values, ceiling):
    return jnp.round(values * (PEAK / jnp.maximum(ceiling, 1e-30))).astype(jnp.int32).astype(jnp.int16)


def dequantize(codes, ceiling):
    return codes.astype(jnp.int32).astype(jnp.float32) * (ceiling * (1.0 / PEAK))


def turn(phase):
    count = jnp.round(phase * 0.6366197723675814)
    rest = ((phase - count * 1.5703125) - count * 4.837512969970703125e-4) - count * 7.54978995489188216e-8
    square = rest * rest
    sine = rest + rest * square * (
        (-1.9515295891e-4 * square + 8.3321608736e-3) * square - 1.6666654611e-1
    )
    cosine = (1.0 - 0.5 * square) + square * square * (
        (2.443315711809948e-5 * square - 1.388731625493765e-3) * square + 4.166664568298827e-2
    )
    quarter = count.astype(jnp.int32)
    odd = (quarter & 1) == 1
    real, imag = jnp.where(odd, sine, cosine), jnp.where(odd, cosine, sine)
    real = jnp.where(((quarter + 1) & 2) == 2, -real, real)
    imag = jnp.where((quarter & 2) == 2, -imag, imag)
    return real, imag


def disperse(x, h_real, h_imag, left_ref, right_ref, twist_ref):
    root = twist_ref.shape[1]
    cos_twist, sin_twist = twist_ref[0], twist_ref[1]
    a = dot3(left_ref[0], left_ref[1], *split(x))
    a_real, a_imag = a[:root], a[root:]
    b = jnp.concatenate(
        [a_real * cos_twist + a_imag * sin_twist, a_imag * cos_twist - a_real * sin_twist], axis=1
    )
    s = dot3(*split(b), right_ref[0], right_ref[1])
    s_real, s_imag = s[:, :root], s[:, root:]
    c = jnp.concatenate([s_real * h_real - s_imag * h_imag, s_real * h_imag + s_imag * h_real], axis=1)
    d = dot3(*split(c), left_ref[0], left_ref[1])
    d_real, d_imag = d[:, :root], d[:, root:]
    e = jnp.concatenate(
        [d_real * cos_twist - d_imag * sin_twist, d_imag * cos_twist + d_real * sin_twist], axis=0
    )
    return dot3(right_ref[0], right_ref[1], *split(e)) * (1.0 / (root * root))


def series_kernel(
    n_low,
    n_high,
    chunks,
    dm_ref,
    delay_ref,
    raw_hbm,
    weight_ref,
    left_hbm,
    right_hbm,
    twist_hbm,
    out_ref,
    peak_ref,
    *scratch,
):
    got, partial, codes, landed, scale, scale_in = (scratch[2 * i : 2 * i + 2] for i in range(6))
    gather_send, gather_recv, sum_send, sum_recv, scale_send, scale_recv = (
        scratch[12 + 2 * i : 14 + 2 * i] for i in range(6)
    )
    chirp, flat, ready, ready_peak, middle, middle_peak = scratch[24:30]
    weight_refs, volt_ref, source, moved, signed = scratch[39:41], *scratch[41:45]
    left_ref, right_ref, twist_ref, table_sem, raw_ref, raw_sem = scratch[45:]
    tables = [
        pltpu.make_async_copy(left_hbm, left_ref, table_sem.at[0]),
        pltpu.make_async_copy(right_hbm, right_ref, table_sem.at[1]),
        pltpu.make_async_copy(twist_hbm, twist_ref, table_sem.at[2]),
    ]
    move_send, move_recv, peak_send, peak_recv, pass_send, pass_recv, last_send, last_recv, own_sem = scratch[30:39]
    n_sta, n_beams, n_sub, _, rows_out, _ = out_ref.shape
    root = twist_hbm.shape[1]
    n_dev = n_sub * n_sta
    sub, sta = lax.axis_index("sub"), lax.axis_index("sta")
    sub_peer = lambda k: lax.rem(sub + k, n_sub)
    sta_peer = lambda k: lax.rem(sta + k, n_sta)
    half = root // 2
    pitch = partial[0].shape[1] // weight_refs[0].shape[0]
    blocks = volt_ref.shape[0] // 2 // chunks

    quarter = raw_hbm.shape[2] // 4

    def fetch(index):
        span = pl.ds(index * quarter, quarter)
        return pltpu.make_async_copy(raw_hbm.at[:, :, span], raw_ref.at[:, :, span], raw_sem.at[index])

    for index in (3, 0, 1, 2):
        fetch(index).start()
    for copy in tables:
        copy.start()

    barrier = pltpu.get_barrier_semaphore()

    for k in range(1, n_sub):
        pl.semaphore_signal(barrier, inc=1, device_id=(sub_peer(k), sta), device_id_type=MESH)
    for k in range(1, n_sta):
        pl.semaphore_signal(barrier, inc=1, device_id=(sub, sta_peer(k)), device_id_type=MESH)

    stations, total_len = raw_hbm.shape[1:]
    depth = 2 * stations
    spread_rows = depth + 4
    all_blocks = total_len // 128

    def unpack(i, carry):
        for u in range(8):
            block = i * 8 + u
            for part in range(2):
                source[pl.ds(block * spread_rows + part * stations, stations), :] = raw_ref[
                    part, :, pl.ds(pl.multiple_of(block * 128, 128), 128)
                ].astype(jnp.float32)
        return carry

    unit = all_blocks // 16

    def unpack_units(first, last):
        lax.fori_loop(first * unit // 8, last * unit // 8, unpack, 0)

    fetch(3).wait()
    unpack_units(12, 16)
    fetch(0).wait()
    unpack_units(0, 1)
    for block in range(16):
        source[pl.ds((all_blocks + block) * spread_rows, depth), :] = source[
            pl.ds(block * spread_rows, depth), :
        ]
    lane = lax.broadcasted_iota(jnp.int32, (8, 128), 1)
    pl.semaphore_wait(barrier, n_sub + n_sta - 2)

    def gather(side, k, chunk):
        return pltpu.make_async_remote_copy(
            src_ref=volt_ref.at[pl.ds((side * chunks + chunk) * blocks, blocks)],
            dst_ref=got[side].at[k, pl.ds(chunk * blocks, blocks)],
            send_sem=gather_send[side].at[k],
            recv_sem=gather_recv[side].at[k, chunk],
            device_id=peers(side, n_low, n_high)[0][k],
            device_id_type=MESH,
        )

    def shift_chunk(chunk, side):
        first = (side * chunks + chunk) * blocks

        def shift_rows(i, carry):
            for u in range(4):
                row = i * 4 + u
                delay = delay_ref[row & (stations - 1)]
                fine, coarse = delay & 127, delay >> 7
                keep_lanes = lane < 128 - fine
                for step in range(0, blocks, 8):
                    start = (first + step - coarse - 1) & (all_blocks - 1)
                    before = source[pl.ds(start * spread_rows + row, 8, stride=spread_rows), :]
                    after = source[pl.ds((start + 1) * spread_rows + row, 8, stride=spread_rows), :]
                    moved[pl.ds(step * spread_rows + row, 8, stride=spread_rows), :] = pltpu.roll(
                        jnp.where(keep_lanes, after, before), fine, 1
                    )
            return carry

        lax.fori_loop(0, depth // 4, shift_rows, 0)

        def pack(i, carry):
            for u in range(8):
                block = i * 8 + u
                volt_ref[first + block] = moved[pl.ds(block * spread_rows, depth), :].astype(volt_ref.dtype)
            return carry

        lax.fori_loop(0, blocks // 8, pack, 0)
        for k in range(len(peers(side, n_low, n_high)[0])):
            gather(side, k, chunk).start()

    shift_chunk(0, 0)
    fetch(1).wait()
    unpack_units(4, 8)
    fetch(2).wait()
    unpack_units(8, 9)
    shift_chunk(0, 1)
    unpack_units(1, 4)
    unpack_units(9, 12)

    def shift_pair(chunk, carry):
        for side in range(2):
            shift_chunk(chunk, side)
        return carry

    lax.fori_loop(1, chunks, shift_pair, 0)

    high, low = sta // n_low, lax.rem(sta, n_low)
    for side, count in enumerate((n_low, n_high)):
        wanted = lax.broadcasted_iota(jnp.int32, (weight_ref.shape[2], count * depth), 0)
        column = lax.broadcasted_iota(jnp.int32, wanted.shape, 1)
        picks = []
        for part in range(2):
            station = jnp.full(wanted.shape, -1, jnp.int32)
            for k in range(count):
                in_row = high * n_low + lax.rem(low - k + n_low, n_low)
                in_column = lax.rem(high - k + n_high, n_high) * n_low + low
                owner = (in_row, in_column)[side]
                begin = k * depth + part * stations
                inside = (column >= begin) & (column < begin + stations)
                station = jnp.where(inside, column - begin + owner * stations, station)
            picks.append((wanted == station).astype(jnp.float32).astype(jnp.bfloat16))
        pick = lambda part, where: jnp.dot(weight_ref[part], picks[where], preferred_element_type=jnp.float32)
        signed[0, :, : count * depth] = pick(0, 0) - pick(1, 1)
        signed[1, :, : count * depth] = pick(1, 0) + pick(0, 1)
        for k in range((n_high, n_low)[side]):
            in_column = lax.rem(high + k, n_high) * n_low + low
            in_row = high * n_low + lax.rem(low + k, n_low)
            owner = (in_column, in_row)[side]
            for part in range(2):
                begin = (k * 2 + part) * n_beams
                weight_refs[side][begin : begin + n_beams, :] = signed[
                    part, pl.ds(owner * n_beams, n_beams), : count * depth
                ]

    for part in range(0, root, 64):
        base_phase = chirp_base(sub, part, 64, root)

        def turns(beam, carry):
            measure = DM_STEP * dm_ref[beam].astype(jnp.float32)
            chirp[beam, 0, part : part + 64], chirp[beam, 1, part : part + 64] = turn(measure * base_phase)
            return carry

        lax.fori_loop(0, n_beams, turns, 0)

    def piece(side, k, part, beam, lanes):
        return partial[side][lanes, pl.ds(((k * 2 + part) * n_beams + beam) * pitch, half), :]

    def exchange(side, k, beam):
        return pltpu.make_async_remote_copy(
            src_ref=codes[side].at[k, beam],
            dst_ref=landed[side].at[k, beam],
            send_sem=sum_send[side].at[k],
            recv_sem=sum_recv[side].at[k, beam],
            device_id=peers(side, n_low, n_high)[1][k],
            device_id_type=MESH,
        )

    def exchange_scale(side, k, beam):
        return pltpu.make_async_remote_copy(
            src_ref=scale[side].at[k, beam],
            dst_ref=scale_in[side].at[k, beam],
            send_sem=scale_send[side].at[k],
            recv_sem=scale_recv[side].at[k, beam],
            device_id=peers(side, n_low, n_high)[1][k],
            device_id_type=MESH,
        )

    def encode_rows(side, k, beam, chunk):
        tall = half // chunks
        rows = pl.ds(chunk * tall, tall)
        for lanes in range(2):
            values = []
            for part in range(2):
                row = (((k + 1) * 2 + part) * n_beams + beam) * pitch + chunk * tall
                values.append(partial[side][lanes, pl.ds(row, tall), :])
            ceiling = jnp.max(jnp.maximum(jnp.abs(values[0]), jnp.abs(values[1])), axis=0, keepdims=True)
            scale[side][k, beam, lanes, chunk : chunk + 1, :] = ceiling
            for part in range(2):
                codes[side][k, beam, part, lanes, rows, :] = quantize(values[part], ceiling)

    def exchange_rows(side, k, chunk):
        rows = pl.ds(chunk * (half // chunks), half // chunks)
        return pltpu.make_async_remote_copy(
            src_ref=codes[side].at[k, 0, :, :, rows],
            dst_ref=landed[side].at[k, 0, :, :, rows],
            send_sem=sum_send[side].at[k],
            recv_sem=sum_recv[side].at[k, 0],
            device_id=peers(side, n_low, n_high)[1][k],
            device_id_type=MESH,
        )

    for chunk in range(chunks):
        for side in range(2):
            members = len(peers(side, n_low, n_high)[0])
            for k in range(members):
                gather(side, k, chunk).wait_recv()
            weights = weight_refs[side][...].astype(jnp.bfloat16)

            def rows(i, carry):
                for u in range(8):
                    row = chunk * (blocks // 2) + i * 8 + u
                    own = side * (volt_ref.shape[0] // 2) + 2 * row
                    tall = [
                        jnp.concatenate([ref[at], ref[at + 1]], axis=1)
                        for ref, at in ((volt_ref, own), *((got[side].at[k], 2 * row) for k in range(members)))
                    ]
                    sums = jnp.dot(weights, jnp.concatenate(tall, axis=0), preferred_element_type=jnp.float32)
                    for lanes in range(2):
                        for base in range(0, weights.shape[0], 8):
                            partial[side][lanes, pl.ds(base * pitch + row, 8, stride=pitch), :] = sums[
                                base : base + 8, lanes * 128 : (lanes + 1) * 128
                            ]
                return carry

            lax.fori_loop(0, blocks // 16, rows, 0)
            for k in range(len(peers(side, n_low, n_high)[1])):
                encode_rows(side, k, 0, chunk)
                exchange_rows(side, k, chunk).start()

    for side in range(2):
        for k in range(len(peers(side, n_low, n_high)[1])):
            exchange_scale(side, k, 0).start()

    def encode(beam, carry):
        for side in range(2):
            for k in range(len(peers(side, n_low, n_high)[1])):
                for chunk in range(chunks):
                    encode_rows(side, k, beam, chunk)
                exchange_scale(side, k, beam).start()
                exchange(side, k, beam).start()
        return carry

    lax.fori_loop(1, n_beams, encode, 0)
    for copy in tables:
        copy.wait()

    def total_of(ref, send_sem, recv_sem):
        return pltpu.make_async_remote_copy(
            src_ref=ref, dst_ref=ref, send_sem=send_sem, recv_sem=recv_sem, device_id=(sub, sta), device_id_type=MESH
        )

    def move(beam, k):
        return pltpu.make_async_remote_copy(
            src_ref=ready.at[sub_peer(k), beam],
            dst_ref=middle.at[beam, sub],
            send_sem=move_send.at[k - 1],
            recv_sem=move_recv.at[beam],
            device_id=(sub_peer(k), sta),
            device_id_type=MESH,
        )

    def move_peak(k):
        return pltpu.make_async_remote_copy(
            src_ref=ready_peak,
            dst_ref=middle_peak.at[sub],
            send_sem=peak_send,
            recv_sem=peak_recv,
            device_id=(sub_peer(k), sta),
            device_id_type=MESH,
        )

    def forward(beam, k):
        return pltpu.make_async_remote_copy(
            src_ref=middle.at[beam, :, sta_peer(k)],
            dst_ref=out_ref.at[sta, beam],
            send_sem=pass_send.at[k - 1],
            recv_sem=pass_recv.at[k - 1],
            device_id=(sub, sta_peer(k)),
            device_id_type=MESH,
        )

    def forward_peak(k):
        return pltpu.make_async_remote_copy(
            src_ref=middle_peak,
            dst_ref=peak_ref.at[sta],
            send_sem=last_send,
            recv_sem=last_recv,
            device_id=(sub, sta_peer(k)),
            device_id_type=MESH,
        )

    def keep(beam):
        return pltpu.make_async_copy(middle.at[beam, :, sta], out_ref.at[sta, beam], own_sem.at[0])

    def finish(beam, carry):
        for side in range(2):
            for k in range(len(peers(side, n_low, n_high)[1])):
                exchange_scale(side, k, beam).wait_recv()
                exchange(side, k, beam).wait_recv()
        quarters = []
        for part in range(2):
            for side in range(2):
                pair = []
                for lanes in range(2):
                    total = piece(side, 0, part, beam, lanes)
                    for k in range(len(peers(side, n_low, n_high)[1])):
                        pieces = []
                        for chunk in range(chunks):
                            tall = half // chunks
                            ceiling = scale_in[side][k, beam, lanes, chunk : chunk + 1, :]
                            rows = pl.ds(chunk * tall, tall)
                            pieces.append(dequantize(landed[side][k, beam, part, lanes, rows, :], ceiling))
                        total = total + jnp.concatenate(pieces, axis=0)
                    pair.append(total)
                quarters.append(jnp.concatenate(pair, axis=1))
        x = jnp.concatenate(quarters, axis=0)
        series = disperse(x, chirp[beam, 0], chirp[beam, 1], left_ref, right_ref, twist_ref)
        for part in range(2):
            for lanes in range(2):
                flat[part, pl.ds(lanes, root, 2), :] = series[
                    part * root : (part + 1) * root, lanes * half : (lanes + 1) * half
                ]
        values = [flat[part] for part in range(2)]
        ceiling = jnp.max(jnp.maximum(jnp.abs(values[0]), jnp.abs(values[1])), axis=0, keepdims=True)
        ready_peak[pl.ds(beam, 1), :] = ceiling
        for part in range(2):
            ready[:, beam, :, part] = quantize(values[part], ceiling).reshape(n_sub, n_sta, rows_out, half)
        middle[beam, sub] = ready[sub, beam]
        for k in range(1, n_sub):
            move(beam, k).start()
        return carry

    lax.fori_loop(0, n_beams, finish, 0)
    middle_peak[sub] = ready_peak[...]
    for k in range(1, n_sub):
        move_peak(k).start()

    def spread(beam, carry):
        total_of(middle.at[beam, pl.ds(0, n_sub - 1)], move_send.at[0], move_recv.at[beam]).wait_recv()
        for k in range(1, n_sta):
            forward(beam, k).start()
        keep(beam).start()
        return carry

    lax.fori_loop(0, n_beams, spread, 0)
    arrived = middle_peak.at[pl.ds(0, n_sub - 1)]
    total_of(arrived, peak_send, peak_recv).wait_recv()
    for k in range(1, n_sta):
        forward_peak(k).start()
    own_peak = pltpu.make_async_copy(middle_peak, peak_ref.at[sta], own_sem.at[1])
    own_peak.start()

    for side in range(2):
        whole = volt_ref.at[pl.ds(side * chunks * blocks, chunks * blocks)]
        for k in range(len(peers(side, n_low, n_high)[0])):
            total_of(whole, gather_send[side].at[k], gather_send[side].at[k]).wait_send()
        for k in range(len(peers(side, n_low, n_high)[1])):
            total_of(codes[side].at[k], sum_send[side].at[k], sum_send[side].at[k]).wait_send()
            total_of(scale[side].at[k], scale_send[side].at[k], scale_send[side].at[k]).wait_send()
    for k in range(1, n_sub):
        total_of(ready.at[sub_peer(k)], move_send.at[k - 1], move_send.at[k - 1]).wait_send()
    total_of(arrived, peak_send, peak_recv).wait_send()
    pltpu.make_async_copy(middle.at[:, :, sta], out_ref.at[sta], own_sem.at[0]).wait()
    own_peak.wait()
    for k in range(1, n_sta):
        total_of(middle.at[:, :, sta_peer(k)], pass_send.at[k - 1], pass_recv.at[k - 1]).wait_send()
        total_of(out_ref.at[sta_peer(k)], pass_send.at[k - 1], pass_recv.at[k - 1]).wait_recv()
    others = peak_ref.at[pl.ds(0, n_sta - 1)]
    total_of(others, last_send, last_recv).wait()


def make_series(dm_index, delays, volts, weights, n_low, n_high, n_sub, root):
    depth, blocks = 2 * volts.shape[1], volts.shape[2] // 128
    spread_rows = depth + 4
    chunks = 8
    n_beams = dm_index.shape[0]
    half = root // 2
    n_sta = n_low * n_high
    rows_out = 2 * root // (n_sub * n_sta)
    tables = dft_tables(root)
    vmem = pl.BlockSpec(memory_space=pltpu.VMEM)
    hbm = pl.BlockSpec(memory_space=pltpu.HBM)
    pitch = half + 4
    dma = pltpu.SemaphoreType.DMA
    groups = ((n_low, n_high), (n_high, n_low))
    per_side = lambda make: [make(*group) for group in groups]
    return pl.pallas_call(
        functools.partial(series_kernel, n_low, n_high, chunks),
        in_specs=[*[pl.BlockSpec(memory_space=pltpu.SMEM)] * 2, hbm, vmem, *[hbm] * 3],
        out_specs=(hbm, hbm),
        out_shape=(
            jax.ShapeDtypeStruct((n_sta, n_beams, n_sub, 2, rows_out, 128), jnp.int16),
            jax.ShapeDtypeStruct((n_sta, n_sub, n_beams, 128), jnp.float32),
        ),
        scratch_shapes=[
            *per_side(lambda g, r: pltpu.VMEM((g - 1, blocks // 2, depth, 128), jnp.bfloat16)),
            *per_side(lambda g, r: pltpu.VMEM((2, r * 2 * n_beams * pitch, 128), jnp.float32)),
            *per_side(lambda g, r: pltpu.VMEM((r - 1, n_beams, 2, 2, half, 128), jnp.int16)),
            *per_side(lambda g, r: pltpu.VMEM((r - 1, n_beams, 2, 2, half, 128), jnp.int16)),
            *per_side(lambda g, r: pltpu.VMEM((r - 1, n_beams, 2, 8, 128), jnp.float32)),
            *per_side(lambda g, r: pltpu.VMEM((r - 1, n_beams, 2, 8, 128), jnp.float32)),
            *per_side(lambda g, r: dma((g - 1,))),
            *per_side(lambda g, r: dma((g - 1, chunks))),
            *per_side(lambda g, r: dma((r - 1,))),
            *per_side(lambda g, r: dma((r - 1, n_beams))),
            *per_side(lambda g, r: dma((r - 1,))),
            *per_side(lambda g, r: dma((r - 1, n_beams))),
            pltpu.VMEM((n_beams, 2, root, root), jnp.float32),
            pltpu.VMEM((2, 2 * root, 128), jnp.float32),
            pltpu.VMEM((n_sub, n_beams, n_sta, 2, rows_out, 128), jnp.int16),
            pltpu.VMEM((n_beams, 128), jnp.float32),
            pltpu.VMEM((n_beams, n_sub, n_sta, 2, rows_out, 128), jnp.int16),
            pltpu.VMEM((n_sub, n_beams, 128), jnp.float32),
            dma((n_sub - 1,)),
            dma((n_beams,)),
            dma,
            dma,
            dma((n_sta - 1,)),
            dma((n_sta - 1,)),
            dma,
            dma,
            dma((2,)),
            *per_side(lambda g, r: pltpu.VMEM((r * 2 * n_beams, g * depth), jnp.float32)),
            pltpu.VMEM((blocks, depth, 128), jnp.bfloat16),
            pltpu.VMEM(((blocks + 16) * spread_rows, 128), jnp.float32),
            pltpu.VMEM((blocks // 2 // chunks * spread_rows, 128), jnp.float32),
            pltpu.VMEM((2, weights.shape[1], 128), jnp.float32),
            *[pltpu.VMEM(table.shape, table.dtype) for table in tables],
            dma((3,)),
            pltpu.VMEM(volts.shape, volts.dtype),
            dma((4,)),
        ],
        compiler_params=pltpu.CompilerParams(
            collective_id=0, has_side_effects=True, vmem_limit_bytes=60 * 1024 * 1024
        ),
        cost_estimate=pl.CostEstimate(
            flops=8 * n_beams * depth * blocks * 128, bytes_accessed=2 * volts.size, transcendentals=0
        ),
    )(dm_index[:, 0], delays, volts, weights, *tables)


def unpack_kernel(codes_ref, peak_ref, out_ref, power_ref):
    n_sub, _, n_beams = out_ref.shape[:3]
    for beam in range(n_beams):
        power = jnp.zeros(power_ref.shape[1:], jnp.float32)
        for sub in range(n_sub):
            for part in range(2):
                values = dequantize(codes_ref[0, beam, sub, part], peak_ref[0, sub, beam : beam + 1, :])
                out_ref[sub, part, beam] = values
                power = power + values * values
        power_ref[beam] = power * (1.0 / n_sub)


def unpack_series(codes, peak):
    n_sta, n_beams, n_sub, _, rows, lanes = codes.shape
    return pl.pallas_call(
        unpack_kernel,
        grid=(n_sta,),
        in_specs=[
            pl.BlockSpec((1, n_beams, n_sub, 2, rows, lanes), lambda i: (i, 0, 0, 0, 0, 0)),
            pl.BlockSpec((1, n_sub, n_beams, lanes), lambda i: (i, 0, 0, 0)),
        ],
        out_specs=[
            pl.BlockSpec((n_sub, 2, n_beams, rows, lanes), lambda i: (0, 0, i, 0, 0)),
            pl.BlockSpec((n_beams, rows, lanes), lambda i: (i, 0, 0)),
        ],
        out_shape=[
            jax.ShapeDtypeStruct((n_sub, 2, n_sta * n_beams, rows, lanes), jnp.float32),
            jax.ShapeDtypeStruct((n_sta * n_beams, rows, lanes), jnp.float32),
        ],
    )(codes, peak)


def shards(voltages, beam_weights, station_delays, dm_index):
    sub_dev = voltages.shape[0]
    total_len = voltages.shape[3]
    local_beams = dm_index.shape[0]
    trials = dm_index.shape[1]
    root_len = int(round(total_len**0.5))
    n_sub = lax.axis_size("sub")
    n_sta = lax.axis_size("sta")
    assert sub_dev == 1 and trials == 1 and root_len * root_len == total_len
    n_low = 2 if n_sta % 2 == 0 else 1
    n_high = n_sta // n_low
    codes, peak = make_series(
        dm_index, station_delays, voltages[0], beam_weights[0], n_low, n_high, n_sub, root_len
    )
    moved, intensity = unpack_series(codes, peak)
    return (moved.reshape(*moved.shape[:3], 1, -1), intensity.reshape(intensity.shape[0], 1, -1))


def solution(mesh):
    return jax.shard_map(
        shards,
        mesh=mesh,
        in_specs=(
            P("sub", None, "sta", None),
            P("sub", None, None, None),
            P("sta"),
            P("sta", None),
        ),
        out_specs=(P(None, None, None, None, ("sub", "sta")), P(None, None, ("sub", "sta"))),
        check_vma=False,
    )
```

```python
import functools

import jax
import jax.numpy as jnp
import numpy as np
from jax import lax
from jax.experimental import pallas as pl
from jax.experimental.pallas import tpu as pltpu
from jax.sharding import PartitionSpec as P


TWO_PI = 6.283185307179586
DISPERSION = 4148808000.0
DM_STEP = 10.0
BASE_FREQ = 120.0
CHANNEL_WIDTH = 0.1953125


def dft_tables(root_len):
    total_len = root_len * root_len
    product = np.outer(np.arange(root_len), np.arange(root_len))
    root_angle = 2 * np.pi * (product % root_len) / root_len
    cos_root, sin_root = np.cos(root_angle), np.sin(root_angle)
    left = np.block([[cos_root, sin_root], [-sin_root, cos_root]]).astype(np.float32)
    high = left.astype(jnp.bfloat16)
    low = (left - high.astype(np.float32)).astype(jnp.bfloat16)
    twist_angle = 2 * np.pi * product / total_len
    twist = np.stack([np.cos(twist_angle), np.sin(twist_angle)]).astype(np.float32)
    return np.stack([high, low]), np.stack([high.T, low.T]), twist


def chirp_base(subband, begin, rows, root_len):
    total_len = root_len * root_len
    first = lax.broadcasted_iota(jnp.int32, (rows, root_len), 0) + begin
    second = lax.broadcasted_iota(jnp.int32, (rows, root_len), 1)
    positions = first + root_len * second
    signed_bin = jnp.where(positions < total_len // 2, positions, positions - total_len)
    offset = CHANNEL_WIDTH * signed_bin.astype(jnp.float32) / total_len
    band = jnp.full((rows, root_len), subband, jnp.int32).astype(jnp.float32)
    centre = BASE_FREQ + CHANNEL_WIDTH * (band + 0.5)
    return TWO_PI * DISPERSION * offset * offset / (centre * centre * (centre + offset))


def split(values):
    high = values.astype(jnp.bfloat16)
    return high, (values - high.astype(jnp.float32)).astype(jnp.bfloat16)


def dot3(a_high, a_low, b_high, b_low):
    dot = functools.partial(jnp.dot, preferred_element_type=jnp.float32)
    return dot(a_high, b_high) + (dot(a_high, b_low) + dot(a_low, b_high))


MESH = pl.DeviceIdType.MESH
PEAK = 32767.0


def peers(side, n_low, n_high):
    sub, sta = lax.axis_index("sub"), lax.axis_index("sta")
    high, low = sta // n_low, lax.rem(sta, n_low)
    along = (
        [(sub, high * n_low + lax.rem(low + k, n_low)) for k in range(1, n_low)],
        [(sub, lax.rem(high + k, n_high) * n_low + low) for k in range(1, n_high)],
    )
    return along[side], along[1 - side]


def quantize(values, ceiling):
    return jnp.round(values * (PEAK / jnp.maximum(ceiling, 1e-30))).astype(jnp.int32).astype(jnp.int16)


def dequantize(codes, ceiling):
    return codes.astype(jnp.int32).astype(jnp.float32) * (ceiling * (1.0 / PEAK))


def turn(phase):
    count = jnp.round(phase * 0.6366197723675814)
    rest = ((phase - count * 1.5703125) - count * 4.837512969970703125e-4) - count * 7.54978995489188216e-8
    square = rest * rest
    sine = rest + rest * square * (
        (-1.9515295891e-4 * square + 8.3321608736e-3) * square - 1.6666654611e-1
    )
    cosine = (1.0 - 0.5 * square) + square * square * (
        (2.443315711809948e-5 * square - 1.388731625493765e-3) * square + 4.166664568298827e-2
    )
    quarter = count.astype(jnp.int32)
    odd = (quarter & 1) == 1
    real, imag = jnp.where(odd, sine, cosine), jnp.where(odd, cosine, sine)
    real = jnp.where(((quarter + 1) & 2) == 2, -real, real)
    imag = jnp.where((quarter & 2) == 2, -imag, imag)
    return real, imag


def disperse(x, h_real, h_imag, left_ref, right_ref, twist_ref):
    root = twist_ref.shape[1]
    cos_twist, sin_twist = twist_ref[0], twist_ref[1]
    a = dot3(left_ref[0], left_ref[1], *split(x))
    a_real, a_imag = a[:root], a[root:]
    b = jnp.concatenate(
        [a_real * cos_twist + a_imag * sin_twist, a_imag * cos_twist - a_real * sin_twist], axis=1
    )
    s = dot3(*split(b), right_ref[0], right_ref[1])
    s_real, s_imag = s[:, :root], s[:, root:]
    c = jnp.concatenate([s_real * h_real - s_imag * h_imag, s_real * h_imag + s_imag * h_real], axis=1)
    d = dot3(*split(c), left_ref[0], left_ref[1])
    d_real, d_imag = d[:, :root], d[:, root:]
    e = jnp.concatenate(
        [d_real * cos_twist - d_imag * sin_twist, d_imag * cos_twist + d_real * sin_twist], axis=0
    )
    return dot3(right_ref[0], right_ref[1], *split(e)) * (1.0 / (root * root))


def series_kernel(
    n_low,
    n_high,
    chunks,
    dm_ref,
    delay_ref,
    raw_hbm,
    weight_ref,
    left_hbm,
    right_hbm,
    twist_hbm,
    out_ref,
    peak_ref,
    *scratch,
):
    got, partial, codes, landed, scale, scale_in = (scratch[2 * i : 2 * i + 2] for i in range(6))
    gather_send, gather_recv, sum_send, sum_recv, scale_send, scale_recv = (
        scratch[12 + 2 * i : 14 + 2 * i] for i in range(6)
    )
    chirp, flat, ready, ready_peak, middle, middle_peak = scratch[24:30]
    weight_refs, volt_ref, source, moved, signed = scratch[39:41], *scratch[41:45]
    left_ref, right_ref, twist_ref, table_sem, raw_ref, raw_sem = scratch[45:]
    tables = [
        pltpu.make_async_copy(left_hbm, left_ref, table_sem.at[0]),
        pltpu.make_async_copy(right_hbm, right_ref, table_sem.at[1]),
        pltpu.make_async_copy(twist_hbm, twist_ref, table_sem.at[2]),
    ]
    move_send, move_recv, peak_send, peak_recv, pass_send, pass_recv, last_send, last_recv, own_sem = scratch[30:39]
    n_sta, n_beams, n_sub, _, rows_out, _ = out_ref.shape
    root = twist_hbm.shape[1]
    n_dev = n_sub * n_sta
    sub, sta = lax.axis_index("sub"), lax.axis_index("sta")
    sub_peer = lambda k: lax.rem(sub + k, n_sub)
    sta_peer = lambda k: lax.rem(sta + k, n_sta)
    half = root // 2
    pitch = partial[0].shape[1] // weight_refs[0].shape[0]
    blocks = volt_ref.shape[0] // 2 // chunks

    quarter = raw_hbm.shape[2] // 4

    def fetch(index):
        span = pl.ds(index * quarter, quarter)
        return pltpu.make_async_copy(raw_hbm.at[:, :, span], raw_ref.at[:, :, span], raw_sem.at[index])

    for index in (3, 0, 1, 2):
        fetch(index).start()
    for copy in tables:
        copy.start()

    barrier = pltpu.get_barrier_semaphore()

    for k in range(1, n_sub):
        pl.semaphore_signal(barrier, inc=1, device_id=(sub_peer(k), sta), device_id_type=MESH)
    for k in range(1, n_sta):
        pl.semaphore_signal(barrier, inc=1, device_id=(sub, sta_peer(k)), device_id_type=MESH)

    stations, total_len = raw_hbm.shape[1:]
    depth = 2 * stations
    spread_rows = depth + 4
    all_blocks = total_len // 128

    def unpack(i, carry):
        for u in range(8):
            block = i * 8 + u
            for part in range(2):
                source[pl.ds(block * spread_rows + part * stations, stations), :] = raw_ref[
                    part, :, pl.ds(pl.multiple_of(block * 128, 128), 128)
                ].astype(jnp.float32)
        return carry

    unit = all_blocks // 16

    def unpack_units(first, last):
        lax.fori_loop(first * unit // 8, last * unit // 8, unpack, 0)

    fetch(3).wait()
    unpack_units(12, 16)
    fetch(0).wait()
    unpack_units(0, 1)
    for block in range(16):
        source[pl.ds((all_blocks + block) * spread_rows, depth), :] = source[
            pl.ds(block * spread_rows, depth), :
        ]
    lane = lax.broadcasted_iota(jnp.int32, (8, 128), 1)
    pl.semaphore_wait(barrier, n_sub + n_sta - 2)

    def gather(side, k, chunk):
        return pltpu.make_async_remote_copy(
            src_ref=volt_ref.at[pl.ds((side * chunks + chunk) * blocks, blocks)],
            dst_ref=got[side].at[k, pl.ds(chunk * blocks, blocks)],
            send_sem=gather_send[side].at[k],
            recv_sem=gather_recv[side].at[k, chunk],
            device_id=peers(side, n_low, n_high)[0][k],
            device_id_type=MESH,
        )

    def shift_chunk(chunk, side):
        first = (side * chunks + chunk) * blocks

        def shift_rows(i, carry):
            for u in range(4):
                row = i * 4 + u
                delay = delay_ref[row & (stations - 1)]
                fine, coarse = delay & 127, delay >> 7
                keep_lanes = lane < 128 - fine
                for step in range(0, blocks, 8):
                    start = (first + step - coarse - 1) & (all_blocks - 1)
                    before = source[pl.ds(start * spread_rows + row, 8, stride=spread_rows), :]
                    after = source[pl.ds((start + 1) * spread_rows + row, 8, stride=spread_rows), :]
                    moved[pl.ds(step * spread_rows + row, 8, stride=spread_rows), :] = pltpu.roll(
                        jnp.where(keep_lanes, after, before), fine, 1
                    )
            return carry

        lax.fori_loop(0, depth // 4, shift_rows, 0)

        def pack(i, carry):
            for u in range(8):
                block = i * 8 + u
                volt_ref[first + block] = moved[pl.ds(block * spread_rows, depth), :].astype(volt_ref.dtype)
            return carry

        lax.fori_loop(0, blocks // 8, pack, 0)
        for k in range(len(peers(side, n_low, n_high)[0])):
            gather(side, k, chunk).start()

    shift_chunk(0, 0)
    fetch(1).wait()
    unpack_units(4, 8)
    fetch(2).wait()
    unpack_units(8, 9)
    shift_chunk(0, 1)
    unpack_units(1, 4)
    unpack_units(9, 12)

    def shift_pair(chunk, carry):
        for side in range(2):
            shift_chunk(chunk, side)
        return carry

    lax.fori_loop(1, chunks, shift_pair, 0)

    high, low = sta // n_low, lax.rem(sta, n_low)
    for side, count in enumerate((n_low, n_high)):
        wanted = lax.broadcasted_iota(jnp.int32, (weight_ref.shape[2], count * depth), 0)
        column = lax.broadcasted_iota(jnp.int32, wanted.shape, 1)
        picks = []
        for part in range(2):
            station = jnp.full(wanted.shape, -1, jnp.int32)
            for k in range(count):
                in_row = high * n_low + lax.rem(low - k + n_low, n_low)
                in_column = lax.rem(high - k + n_high, n_high) * n_low + low
                owner = (in_row, in_column)[side]
                begin = k * depth + part * stations
                inside = (column >= begin) & (column < begin + stations)
                station = jnp.where(inside, column - begin + owner * stations, station)
            picks.append((wanted == station).astype(jnp.float32).astype(jnp.bfloat16))
        pick = lambda part, where: jnp.dot(weight_ref[part], picks[where], preferred_element_type=jnp.float32)
        signed[0, :, : count * depth] = pick(0, 0) - pick(1, 1)
        signed[1, :, : count * depth] = pick(1, 0) + pick(0, 1)
        for k in range((n_high, n_low)[side]):
            in_column = lax.rem(high + k, n_high) * n_low + low
            in_row = high * n_low + lax.rem(low + k, n_low)
            owner = (in_column, in_row)[side]
            for part in range(2):
                begin = (k * 2 + part) * n_beams
                weight_refs[side][begin : begin + n_beams, :] = signed[
                    part, pl.ds(owner * n_beams, n_beams), : count * depth
                ]

    for part in range(0, root, 64):
        base_phase = chirp_base(sub, part, 64, root)

        def turns(beam, carry):
            measure = DM_STEP * dm_ref[beam].astype(jnp.float32)
            chirp[beam, 0, part : part + 64], chirp[beam, 1, part : part + 64] = turn(measure * base_phase)
            return carry

        lax.fori_loop(0, n_beams, turns, 0)

    def piece(side, k, part, beam, lanes):
        return partial[side][lanes, pl.ds(((k * 2 + part) * n_beams + beam) * pitch, half), :]

    def exchange(side, k, beam):
        return pltpu.make_async_remote_copy(
            src_ref=codes[side].at[k, beam],
            dst_ref=landed[side].at[k, beam],
            send_sem=sum_send[side].at[k],
            recv_sem=sum_recv[side].at[k, beam],
            device_id=peers(side, n_low, n_high)[1][k],
            device_id_type=MESH,
        )

    def exchange_scale(side, k, beam):
        return pltpu.make_async_remote_copy(
            src_ref=scale[side].at[k, beam],
            dst_ref=scale_in[side].at[k, beam],
            send_sem=scale_send[side].at[k],
            recv_sem=scale_recv[side].at[k, beam],
            device_id=peers(side, n_low, n_high)[1][k],
            device_id_type=MESH,
        )

    def encode_rows(side, k, beam, chunk):
        tall = half // chunks
        rows = pl.ds(chunk * tall, tall)
        for lanes in range(2):
            values = []
            for part in range(2):
                row = (((k + 1) * 2 + part) * n_beams + beam) * pitch + chunk * tall
                values.append(partial[side][lanes, pl.ds(row, tall), :])
            ceiling = jnp.max(jnp.maximum(jnp.abs(values[0]), jnp.abs(values[1])), axis=0, keepdims=True)
            scale[side][k, beam, lanes, chunk : chunk + 1, :] = ceiling
            for part in range(2):
                codes[side][k, beam, part, lanes, rows, :] = quantize(values[part], ceiling)

    def exchange_rows(side, k, chunk):
        rows = pl.ds(chunk * (half // chunks), half // chunks)
        return pltpu.make_async_remote_copy(
            src_ref=codes[side].at[k, 0, :, :, rows],
            dst_ref=landed[side].at[k, 0, :, :, rows],
            send_sem=sum_send[side].at[k],
            recv_sem=sum_recv[side].at[k, 0],
            device_id=peers(side, n_low, n_high)[1][k],
            device_id_type=MESH,
        )

    for chunk in range(chunks):
        for side in range(2):
            members = len(peers(side, n_low, n_high)[0])
            for k in range(members):
                gather(side, k, chunk).wait_recv()
            weights = weight_refs[side][...].astype(jnp.bfloat16)

            def rows(i, carry):
                for u in range(8):
                    row = chunk * (blocks // 2) + i * 8 + u
                    own = side * (volt_ref.shape[0] // 2) + 2 * row
                    tall = [
                        jnp.concatenate([ref[at], ref[at + 1]], axis=1)
                        for ref, at in ((volt_ref, own), *((got[side].at[k], 2 * row) for k in range(members)))
                    ]
                    sums = jnp.dot(weights, jnp.concatenate(tall, axis=0), preferred_element_type=jnp.float32)
                    for lanes in range(2):
                        for base in range(0, weights.shape[0], 8):
                            partial[side][lanes, pl.ds(base * pitch + row, 8, stride=pitch), :] = sums[
                                base : base + 8, lanes * 128 : (lanes + 1) * 128
                            ]
                return carry

            lax.fori_loop(0, blocks // 16, rows, 0)
            for k in range(len(peers(side, n_low, n_high)[1])):
                encode_rows(side, k, 0, chunk)
                exchange_rows(side, k, chunk).start()

    for side in range(2):
        for k in range(len(peers(side, n_low, n_high)[1])):
            exchange_scale(side, k, 0).start()

    def encode(beam, carry):
        for side in range(2):
            for k in range(len(peers(side, n_low, n_high)[1])):
                for chunk in range(chunks):
                    encode_rows(side, k, beam, chunk)
                exchange_scale(side, k, beam).start()
                exchange(side, k, beam).start()
        return carry

    lax.fori_loop(1, n_beams, encode, 0)
    for copy in tables:
        copy.wait()

    def total_of(ref, send_sem, recv_sem):
        return pltpu.make_async_remote_copy(
            src_ref=ref, dst_ref=ref, send_sem=send_sem, recv_sem=recv_sem, device_id=(sub, sta), device_id_type=MESH
        )

    def move(beam, k):
        return pltpu.make_async_remote_copy(
            src_ref=ready.at[sub_peer(k), beam],
            dst_ref=middle.at[beam, sub],
            send_sem=move_send.at[k - 1],
            recv_sem=move_recv.at[beam],
            device_id=(sub_peer(k), sta),
            device_id_type=MESH,
        )

    def move_peak(k):
        return pltpu.make_async_remote_copy(
            src_ref=ready_peak,
            dst_ref=middle_peak.at[sub],
            send_sem=peak_send,
            recv_sem=peak_recv,
            device_id=(sub_peer(k), sta),
            device_id_type=MESH,
        )

    def forward(beam, k):
        return pltpu.make_async_remote_copy(
            src_ref=middle.at[beam, :, sta_peer(k)],
            dst_ref=out_ref.at[sta, beam],
            send_sem=pass_send.at[k - 1],
            recv_sem=pass_recv.at[k - 1],
            device_id=(sub, sta_peer(k)),
            device_id_type=MESH,
        )

    def forward_peak(k):
        return pltpu.make_async_remote_copy(
            src_ref=middle_peak,
            dst_ref=peak_ref.at[sta],
            send_sem=last_send,
            recv_sem=last_recv,
            device_id=(sub, sta_peer(k)),
            device_id_type=MESH,
        )

    def keep(beam):
        return pltpu.make_async_copy(middle.at[beam, :, sta], out_ref.at[sta, beam], own_sem.at[0])

    lag = 5

    def spread(beam, carry):
        total_of(middle.at[beam, pl.ds(0, n_sub - 1)], move_send.at[0], move_recv.at[beam]).wait_recv()
        for k in range(1, n_sta):
            forward(beam, k).start()
        keep(beam).start()
        return carry

    def finish(beam, carry):
        for side in range(2):
            for k in range(len(peers(side, n_low, n_high)[1])):
                exchange_scale(side, k, beam).wait_recv()
                exchange(side, k, beam).wait_recv()
        quarters = []
        for part in range(2):
            for side in range(2):
                pair = []
                for lanes in range(2):
                    total = piece(side, 0, part, beam, lanes)
                    for k in range(len(peers(side, n_low, n_high)[1])):
                        pieces = []
                        for chunk in range(chunks):
                            tall = half // chunks
                            ceiling = scale_in[side][k, beam, lanes, chunk : chunk + 1, :]
                            rows = pl.ds(chunk * tall, tall)
                            pieces.append(dequantize(landed[side][k, beam, part, lanes, rows, :], ceiling))
                        total = total + jnp.concatenate(pieces, axis=0)
                    pair.append(total)
                quarters.append(jnp.concatenate(pair, axis=1))
        x = jnp.concatenate(quarters, axis=0)
        series = disperse(x, chirp[beam, 0], chirp[beam, 1], left_ref, right_ref, twist_ref)
        for part in range(2):
            for lanes in range(2):
                flat[part, pl.ds(lanes, root, 2), :] = series[
                    part * root : (part + 1) * root, lanes * half : (lanes + 1) * half
                ]
        values = [flat[part] for part in range(2)]
        ceiling = jnp.max(jnp.maximum(jnp.abs(values[0]), jnp.abs(values[1])), axis=0, keepdims=True)
        ready_peak[pl.ds(beam, 1), :] = ceiling
        for part in range(2):
            ready[:, beam, :, part] = quantize(values[part], ceiling).reshape(n_sub, n_sta, rows_out, half)
        middle[beam, sub] = ready[sub, beam]
        for k in range(1, n_sub):
            move(beam, k).start()

        @pl.when(beam >= lag)
        def _():
            spread(beam - lag, 0)

        return carry

    lax.fori_loop(0, n_beams, finish, 0)
    middle_peak[sub] = ready_peak[...]
    for k in range(1, n_sub):
        move_peak(k).start()

    lax.fori_loop(max(n_beams - lag, 0), n_beams, spread, 0)
    arrived = middle_peak.at[pl.ds(0, n_sub - 1)]
    total_of(arrived, peak_send, peak_recv).wait_recv()
    for k in range(1, n_sta):
        forward_peak(k).start()
    own_peak = pltpu.make_async_copy(middle_peak, peak_ref.at[sta], own_sem.at[1])
    own_peak.start()

    for side in range(2):
        whole = volt_ref.at[pl.ds(side * chunks * blocks, chunks * blocks)]
        for k in range(len(peers(side, n_low, n_high)[0])):
            total_of(whole, gather_send[side].at[k], gather_send[side].at[k]).wait_send()
        for k in range(len(peers(side, n_low, n_high)[1])):
            total_of(codes[side].at[k], sum_send[side].at[k], sum_send[side].at[k]).wait_send()
            total_of(scale[side].at[k], scale_send[side].at[k], scale_send[side].at[k]).wait_send()
    for k in range(1, n_sub):
        total_of(ready.at[sub_peer(k)], move_send.at[k - 1], move_send.at[k - 1]).wait_send()
    total_of(arrived, peak_send, peak_recv).wait_send()
    pltpu.make_async_copy(middle.at[:, :, sta], out_ref.at[sta], own_sem.at[0]).wait()
    own_peak.wait()
    for k in range(1, n_sta):
        total_of(middle.at[:, :, sta_peer(k)], pass_send.at[k - 1], pass_recv.at[k - 1]).wait_send()
        total_of(out_ref.at[sta_peer(k)], pass_send.at[k - 1], pass_recv.at[k - 1]).wait_recv()
    others = peak_ref.at[pl.ds(0, n_sta - 1)]
    total_of(others, last_send, last_recv).wait()


def make_series(dm_index, delays, volts, weights, n_low, n_high, n_sub, root):
    depth, blocks = 2 * volts.shape[1], volts.shape[2] // 128
    spread_rows = depth + 4
    chunks = 8
    n_beams = dm_index.shape[0]
    half = root // 2
    n_sta = n_low * n_high
    rows_out = 2 * root // (n_sub * n_sta)
    tables = dft_tables(root)
    vmem = pl.BlockSpec(memory_space=pltpu.VMEM)
    hbm = pl.BlockSpec(memory_space=pltpu.HBM)
    pitch = half + 4
    dma = pltpu.SemaphoreType.DMA
    groups = ((n_low, n_high), (n_high, n_low))
    per_side = lambda make: [make(*group) for group in groups]
    return pl.pallas_call(
        functools.partial(series_kernel, n_low, n_high, chunks),
        in_specs=[*[pl.BlockSpec(memory_space=pltpu.SMEM)] * 2, hbm, vmem, *[hbm] * 3],
        out_specs=(hbm, hbm),
        out_shape=(
            jax.ShapeDtypeStruct((n_sta, n_beams, n_sub, 2, rows_out, 128), jnp.int16),
            jax.ShapeDtypeStruct((n_sta, n_sub, n_beams, 128), jnp.float32),
        ),
        scratch_shapes=[
            *per_side(lambda g, r: pltpu.VMEM((g - 1, blocks // 2, depth, 128), jnp.bfloat16)),
            *per_side(lambda g, r: pltpu.VMEM((2, r * 2 * n_beams * pitch, 128), jnp.float32)),
            *per_side(lambda g, r: pltpu.VMEM((r - 1, n_beams, 2, 2, half, 128), jnp.int16)),
            *per_side(lambda g, r: pltpu.VMEM((r - 1, n_beams, 2, 2, half, 128), jnp.int16)),
            *per_side(lambda g, r: pltpu.VMEM((r - 1, n_beams, 2, 8, 128), jnp.float32)),
            *per_side(lambda g, r: pltpu.VMEM((r - 1, n_beams, 2, 8, 128), jnp.float32)),
            *per_side(lambda g, r: dma((g - 1,))),
            *per_side(lambda g, r: dma((g - 1, chunks))),
            *per_side(lambda g, r: dma((r - 1,))),
            *per_side(lambda g, r: dma((r - 1, n_beams))),
            *per_side(lambda g, r: dma((r - 1,))),
            *per_side(lambda g, r: dma((r - 1, n_beams))),
            pltpu.VMEM((n_beams, 2, root, root), jnp.float32),
            pltpu.VMEM((2, 2 * root, 128), jnp.float32),
            pltpu.VMEM((n_sub, n_beams, n_sta, 2, rows_out, 128), jnp.int16),
            pltpu.VMEM((n_beams, 128), jnp.float32),
            pltpu.VMEM((n_beams, n_sub, n_sta, 2, rows_out, 128), jnp.int16),
            pltpu.VMEM((n_sub, n_beams, 128), jnp.float32),
            dma((n_sub - 1,)),
            dma((n_beams,)),
            dma,
            dma,
            dma((n_sta - 1,)),
            dma((n_sta - 1,)),
            dma,
            dma,
            dma((2,)),
            *per_side(lambda g, r: pltpu.VMEM((r * 2 * n_beams, g * depth), jnp.float32)),
            pltpu.VMEM((blocks, depth, 128), jnp.bfloat16),
            pltpu.VMEM(((blocks + 16) * spread_rows, 128), jnp.float32),
            pltpu.VMEM((blocks // 2 // chunks * spread_rows, 128), jnp.float32),
            pltpu.VMEM((2, weights.shape[1], 128), jnp.float32),
            *[pltpu.VMEM(table.shape, table.dtype) for table in tables],
            dma((3,)),
            pltpu.VMEM(volts.shape, volts.dtype),
            dma((4,)),
        ],
        compiler_params=pltpu.CompilerParams(
            collective_id=0, has_side_effects=True, vmem_limit_bytes=60 * 1024 * 1024
        ),
        cost_estimate=pl.CostEstimate(
            flops=8 * n_beams * depth * blocks * 128, bytes_accessed=2 * volts.size, transcendentals=0
        ),
    )(dm_index[:, 0], delays, volts, weights, *tables)


def unpack_kernel(codes_ref, peak_ref, out_ref, power_ref):
    n_sub, _, n_beams = out_ref.shape[:3]
    for owner in range(codes_ref.shape[0]):
        for beam in range(codes_ref.shape[1]):
            at = owner * codes_ref.shape[1] + beam
            power = jnp.zeros(power_ref.shape[1:], jnp.float32)
            for sub in range(n_sub):
                ceiling = peak_ref[owner, sub, beam : beam + 1, :]
                for part in range(2):
                    values = dequantize(codes_ref[owner, beam, sub, part], ceiling)
                    out_ref[sub, part, at] = values
                    power = power + values * values
            power_ref[at] = power * (1.0 / n_sub)


def unpack_series(codes, peak):
    n_sta, n_beams, n_sub, _, rows, lanes = codes.shape
    group = n_sta // 2
    return pl.pallas_call(
        unpack_kernel,
        grid=(n_sta // group,),
        in_specs=[
            pl.BlockSpec((group, n_beams, n_sub, 2, rows, lanes), lambda i: (i, 0, 0, 0, 0, 0)),
            pl.BlockSpec((group, n_sub, n_beams, lanes), lambda i: (i, 0, 0, 0)),
        ],
        out_specs=[
            pl.BlockSpec((n_sub, 2, group * n_beams, rows, lanes), lambda i: (0, 0, i, 0, 0)),
            pl.BlockSpec((group * n_beams, rows, lanes), lambda i: (i, 0, 0)),
        ],
        out_shape=[
            jax.ShapeDtypeStruct((n_sub, 2, n_sta * n_beams, rows, lanes), jnp.float32),
            jax.ShapeDtypeStruct((n_sta * n_beams, rows, lanes), jnp.float32),
        ],
    )(codes, peak)


def shards(voltages, beam_weights, station_delays, dm_index):
    sub_dev = voltages.shape[0]
    total_len = voltages.shape[3]
    local_beams = dm_index.shape[0]
    trials = dm_index.shape[1]
    root_len = int(round(total_len**0.5))
    n_sub = lax.axis_size("sub")
    n_sta = lax.axis_size("sta")
    assert sub_dev == 1 and trials == 1 and root_len * root_len == total_len
    n_low = 2 if n_sta % 2 == 0 else 1
    n_high = n_sta // n_low
    codes, peak = make_series(
        dm_index, station_delays, voltages[0], beam_weights[0], n_low, n_high, n_sub, root_len
    )
    moved, intensity = unpack_series(codes, peak)
    return (moved.reshape(*moved.shape[:3], 1, -1), intensity.reshape(intensity.shape[0], 1, -1))


def solution(mesh):
    return jax.shard_map(
        shards,
        mesh=mesh,
        in_specs=(
            P("sub", None, "sta", None),
            P("sub", None, None, None),
            P("sta"),
            P("sta", None),
        ),
        out_specs=(P(None, None, None, None, ("sub", "sta")), P(None, None, ("sub", "sta"))),
        check_vma=False,
    )
```

```python
import functools

import jax
import jax.numpy as jnp
import numpy as np
from jax import lax
from jax.experimental import pallas as pl
from jax.experimental.pallas import tpu as pltpu
from jax.sharding import PartitionSpec as P


TWO_PI = 6.283185307179586
DISPERSION = 4148808000.0
DM_STEP = 10.0
BASE_FREQ = 120.0
CHANNEL_WIDTH = 0.1953125


def dft_tables(root_len):
    total_len = root_len * root_len
    product = np.outer(np.arange(root_len), np.arange(root_len))
    root_angle = 2 * np.pi * (product % root_len) / root_len
    cos_root, sin_root = np.cos(root_angle), np.sin(root_angle)
    left = np.block([[cos_root, sin_root], [-sin_root, cos_root]]).astype(np.float32)
    high = left.astype(jnp.bfloat16)
    low = (left - high.astype(np.float32)).astype(jnp.bfloat16)
    twist_angle = 2 * np.pi * product / total_len
    twist = np.stack([np.cos(twist_angle), np.sin(twist_angle)]).astype(np.float32)
    return np.stack([high, low]), np.stack([high.T, low.T]), twist


def chirp_base(subband, begin, rows, root_len):
    total_len = root_len * root_len
    first = lax.broadcasted_iota(jnp.int32, (rows, root_len), 0) + begin
    second = lax.broadcasted_iota(jnp.int32, (rows, root_len), 1)
    positions = first + root_len * second
    signed_bin = jnp.where(positions < total_len // 2, positions, positions - total_len)
    offset = CHANNEL_WIDTH * signed_bin.astype(jnp.float32) / total_len
    band = jnp.full((rows, root_len), subband, jnp.int32).astype(jnp.float32)
    centre = BASE_FREQ + CHANNEL_WIDTH * (band + 0.5)
    return TWO_PI * DISPERSION * offset * offset / (centre * centre * (centre + offset))


def split(values):
    high = values.astype(jnp.bfloat16)
    return high, (values - high.astype(jnp.float32)).astype(jnp.bfloat16)


def dot3(a_high, a_low, b_high, b_low):
    left = jnp.concatenate([a_high, a_high, a_low], axis=1)
    right = jnp.concatenate([b_high, b_low, b_high], axis=0)
    return jnp.dot(left, right, preferred_element_type=jnp.float32)


MESH = pl.DeviceIdType.MESH
PEAK = 32767.0


def peers(side, n_low, n_high):
    sub, sta = lax.axis_index("sub"), lax.axis_index("sta")
    high, low = sta // n_low, lax.rem(sta, n_low)
    along = (
        [(sub, high * n_low + lax.rem(low + k, n_low)) for k in range(1, n_low)],
        [(sub, lax.rem(high + k, n_high) * n_low + low) for k in range(1, n_high)],
    )
    return along[side], along[1 - side]


def quantize(values, ceiling):
    return jnp.round(values * (PEAK / jnp.maximum(ceiling, 1e-30))).astype(jnp.int32).astype(jnp.int16)


def dequantize(codes, ceiling):
    return codes.astype(jnp.int32).astype(jnp.float32) * (ceiling * (1.0 / PEAK))


def turn(phase):
    count = jnp.round(phase * 0.6366197723675814)
    rest = ((phase - count * 1.5703125) - count * 4.837512969970703125e-4) - count * 7.54978995489188216e-8
    square = rest * rest
    sine = rest + rest * square * (
        (-1.9515295891e-4 * square + 8.3321608736e-3) * square - 1.6666654611e-1
    )
    cosine = (1.0 - 0.5 * square) + square * square * (
        (2.443315711809948e-5 * square - 1.388731625493765e-3) * square + 4.166664568298827e-2
    )
    quarter = count.astype(jnp.int32)
    odd = (quarter & 1) == 1
    real, imag = jnp.where(odd, sine, cosine), jnp.where(odd, cosine, sine)
    real = jnp.where(((quarter + 1) & 2) == 2, -real, real)
    imag = jnp.where((quarter & 2) == 2, -imag, imag)
    return real, imag


def disperse(x, h_real, h_imag, left_ref, right_ref, twist_ref):
    root = twist_ref.shape[1]
    cos_twist, sin_twist = twist_ref[0], twist_ref[1]
    a = dot3(left_ref[0], left_ref[1], *split(x))
    a_real, a_imag = a[:root], a[root:]
    b = jnp.concatenate(
        [a_real * cos_twist + a_imag * sin_twist, a_imag * cos_twist - a_real * sin_twist], axis=1
    )
    s = dot3(*split(b), right_ref[0], right_ref[1])
    s_real, s_imag = s[:, :root], s[:, root:]
    c = jnp.concatenate([s_real * h_real - s_imag * h_imag, s_real * h_imag + s_imag * h_real], axis=1)
    d = dot3(*split(c), left_ref[0], left_ref[1])
    d_real, d_imag = d[:, :root], d[:, root:]
    e = jnp.concatenate(
        [d_real * cos_twist - d_imag * sin_twist, d_imag * cos_twist + d_real * sin_twist], axis=0
    )
    return dot3(right_ref[0], right_ref[1], *split(e)) * (1.0 / (root * root))


def series_kernel(
    n_low,
    n_high,
    chunks,
    dm_ref,
    delay_ref,
    raw_hbm,
    weight_ref,
    left_hbm,
    right_hbm,
    twist_hbm,
    out_ref,
    peak_ref,
    *scratch,
):
    got, partial, codes, landed, scale, scale_in = (scratch[2 * i : 2 * i + 2] for i in range(6))
    gather_send, gather_recv, sum_send, sum_recv, scale_send, scale_recv = (
        scratch[12 + 2 * i : 14 + 2 * i] for i in range(6)
    )
    chirp, flat, ready, ready_peak, middle, middle_peak = scratch[24:30]
    weight_refs, volt_ref, source, moved, signed = scratch[39:41], *scratch[41:45]
    left_ref, right_ref, twist_ref, table_sem, raw_ref, raw_sem = scratch[45:]
    tables = [
        pltpu.make_async_copy(left_hbm, left_ref, table_sem.at[0]),
        pltpu.make_async_copy(right_hbm, right_ref, table_sem.at[1]),
        pltpu.make_async_copy(twist_hbm, twist_ref, table_sem.at[2]),
    ]
    move_send, move_recv, peak_send, peak_recv, pass_send, pass_recv, last_send, last_recv, own_sem = scratch[30:39]
    n_sta, n_beams, n_sub, _, rows_out, _ = out_ref.shape
    root = twist_hbm.shape[1]
    n_dev = n_sub * n_sta
    sub, sta = lax.axis_index("sub"), lax.axis_index("sta")
    sub_peer = lambda k: lax.rem(sub + k, n_sub)
    sta_peer = lambda k: lax.rem(sta + k, n_sta)
    half = root // 2
    pitch = partial[0].shape[1] // weight_refs[0].shape[0]
    blocks = volt_ref.shape[0] // 2 // chunks

    quarter = raw_hbm.shape[2] // 4

    def fetch(index):
        span = pl.ds(index * quarter, quarter)
        return pltpu.make_async_copy(raw_hbm.at[:, :, span], raw_ref.at[:, :, span], raw_sem.at[index])

    for index in (3, 0, 1, 2):
        fetch(index).start()
    for copy in tables:
        copy.start()

    barrier = pltpu.get_barrier_semaphore()

    for k in range(1, n_sub):
        pl.semaphore_signal(barrier, inc=1, device_id=(sub_peer(k), sta), device_id_type=MESH)
    for k in range(1, n_sta):
        pl.semaphore_signal(barrier, inc=1, device_id=(sub, sta_peer(k)), device_id_type=MESH)

    stations, total_len = raw_hbm.shape[1:]
    depth = 2 * stations
    spread_rows = depth + 4
    all_blocks = total_len // 128

    def unpack(i, carry):
        for u in range(8):
            block = i * 8 + u
            for part in range(2):
                source[pl.ds(block * spread_rows + part * stations, stations), :] = raw_ref[
                    part, :, pl.ds(pl.multiple_of(block * 128, 128), 128)
                ].astype(jnp.float32)
        return carry

    unit = all_blocks // 16

    def unpack_units(first, last):
        lax.fori_loop(first * unit // 8, last * unit // 8, unpack, 0)

    fetch(3).wait()
    unpack_units(12, 16)
    fetch(0).wait()
    unpack_units(0, 1)
    for block in range(16):
        source[pl.ds((all_blocks + block) * spread_rows, depth), :] = source[
            pl.ds(block * spread_rows, depth), :
        ]
    lane = lax.broadcasted_iota(jnp.int32, (8, 128), 1)
    pl.semaphore_wait(barrier, n_sub + n_sta - 2)

    def gather(side, k, chunk):
        return pltpu.make_async_remote_copy(
            src_ref=volt_ref.at[pl.ds((side * chunks + chunk) * blocks, blocks)],
            dst_ref=got[side].at[k, pl.ds(chunk * blocks, blocks)],
            send_sem=gather_send[side].at[k],
            recv_sem=gather_recv[side].at[k, chunk],
            device_id=peers(side, n_low, n_high)[0][k],
            device_id_type=MESH,
        )

    def shift_chunk(chunk, side):
        first = (side * chunks + chunk) * blocks

        def shift_rows(i, carry):
            for u in range(4):
                row = i * 4 + u
                delay = delay_ref[row & (stations - 1)]
                fine, coarse = delay & 127, delay >> 7
                keep_lanes = lane < 128 - fine
                for step in range(0, blocks, 8):
                    start = (first + step - coarse - 1) & (all_blocks - 1)
                    before = source[pl.ds(start * spread_rows + row, 8, stride=spread_rows), :]
                    after = source[pl.ds((start + 1) * spread_rows + row, 8, stride=spread_rows), :]
                    moved[pl.ds(step * spread_rows + row, 8, stride=spread_rows), :] = pltpu.roll(
                        jnp.where(keep_lanes, after, before), fine, 1
                    )
            return carry

        lax.fori_loop(0, depth // 4, shift_rows, 0)

        def pack(i, carry):
            for u in range(8):
                block = i * 8 + u
                volt_ref[first + block] = moved[pl.ds(block * spread_rows, depth), :].astype(volt_ref.dtype)
            return carry

        lax.fori_loop(0, blocks // 8, pack, 0)
        for k in range(len(peers(side, n_low, n_high)[0])):
            gather(side, k, chunk).start()

    shift_chunk(0, 0)
    fetch(1).wait()
    unpack_units(4, 8)
    fetch(2).wait()
    unpack_units(8, 9)
    shift_chunk(0, 1)
    unpack_units(1, 4)
    unpack_units(9, 12)

    def shift_pair(chunk, carry):
        for side in range(2):
            shift_chunk(chunk, side)
        return carry

    lax.fori_loop(1, chunks, shift_pair, 0)

    high, low = sta // n_low, lax.rem(sta, n_low)
    for side, count in enumerate((n_low, n_high)):
        wanted = lax.broadcasted_iota(jnp.int32, (weight_ref.shape[2], count * depth), 0)
        column = lax.broadcasted_iota(jnp.int32, wanted.shape, 1)
        picks = []
        for part in range(2):
            station = jnp.full(wanted.shape, -1, jnp.int32)
            for k in range(count):
                in_row = high * n_low + lax.rem(low - k + n_low, n_low)
                in_column = lax.rem(high - k + n_high, n_high) * n_low + low
                owner = (in_row, in_column)[side]
                begin = k * depth + part * stations
                inside = (column >= begin) & (column < begin + stations)
                station = jnp.where(inside, column - begin + owner * stations, station)
            picks.append((wanted == station).astype(jnp.float32).astype(jnp.bfloat16))
        pick = lambda part, where: jnp.dot(weight_ref[part], picks[where], preferred_element_type=jnp.float32)
        signed[0, :, : count * depth] = pick(0, 0) - pick(1, 1)
        signed[1, :, : count * depth] = pick(1, 0) + pick(0, 1)
        for k in range((n_high, n_low)[side]):
            in_column = lax.rem(high + k, n_high) * n_low + low
            in_row = high * n_low + lax.rem(low + k, n_low)
            owner = (in_column, in_row)[side]
            for part in range(2):
                begin = (k * 2 + part) * n_beams
                weight_refs[side][begin : begin + n_beams, :] = signed[
                    part, pl.ds(owner * n_beams, n_beams), : count * depth
                ]

    for part in range(0, root, 64):
        base_phase = chirp_base(sub, part, 64, root)

        def turns(beam, carry):
            measure = DM_STEP * dm_ref[beam].astype(jnp.float32)
            chirp[beam, 0, part : part + 64], chirp[beam, 1, part : part + 64] = turn(measure * base_phase)
            return carry

        lax.fori_loop(0, n_beams, turns, 0)

    def piece(side, k, part, beam, lanes):
        return partial[side][lanes, pl.ds(((k * 2 + part) * n_beams + beam) * pitch, half), :]

    def exchange(side, k, beam):
        return pltpu.make_async_remote_copy(
            src_ref=codes[side].at[k, beam],
            dst_ref=landed[side].at[k, beam],
            send_sem=sum_send[side].at[k],
            recv_sem=sum_recv[side].at[k, beam],
            device_id=peers(side, n_low, n_high)[1][k],
            device_id_type=MESH,
        )

    def exchange_scale(side, k, beam):
        return pltpu.make_async_remote_copy(
            src_ref=scale[side].at[k, beam],
            dst_ref=scale_in[side].at[k, beam],
            send_sem=scale_send[side].at[k],
            recv_sem=scale_recv[side].at[k, beam],
            device_id=peers(side, n_low, n_high)[1][k],
            device_id_type=MESH,
        )

    def encode_rows(side, k, beam, chunk):
        tall = half // chunks
        rows = pl.ds(chunk * tall, tall)
        for lanes in range(2):
            values = []
            for part in range(2):
                row = (((k + 1) * 2 + part) * n_beams + beam) * pitch + chunk * tall
                values.append(partial[side][lanes, pl.ds(row, tall), :])
            ceiling = jnp.max(jnp.maximum(jnp.abs(values[0]), jnp.abs(values[1])), axis=0, keepdims=True)
            scale[side][k, beam, lanes, chunk : chunk + 1, :] = ceiling
            for part in range(2):
                codes[side][k, beam, part, lanes, rows, :] = quantize(values[part], ceiling)

    def exchange_rows(side, k, chunk):
        rows = pl.ds(chunk * (half // chunks), half // chunks)
        return pltpu.make_async_remote_copy(
            src_ref=codes[side].at[k, 0, :, :, rows],
            dst_ref=landed[side].at[k, 0, :, :, rows],
            send_sem=sum_send[side].at[k],
            recv_sem=sum_recv[side].at[k, 0],
            device_id=peers(side, n_low, n_high)[1][k],
            device_id_type=MESH,
        )

    for chunk in range(chunks):
        for side in range(2):
            members = len(peers(side, n_low, n_high)[0])
            for k in range(members):
                gather(side, k, chunk).wait_recv()
            weights = weight_refs[side][...].astype(jnp.bfloat16)

            def rows(i, carry):
                for u in range(8):
                    row = chunk * (blocks // 2) + i * 8 + u
                    own = side * (volt_ref.shape[0] // 2) + 2 * row
                    tall = [
                        jnp.concatenate([ref[at], ref[at + 1]], axis=1)
                        for ref, at in ((volt_ref, own), *((got[side].at[k], 2 * row) for k in range(members)))
                    ]
                    sums = jnp.dot(weights, jnp.concatenate(tall, axis=0), preferred_element_type=jnp.float32)
                    for lanes in range(2):
                        for base in range(0, weights.shape[0], 8):
                            partial[side][lanes, pl.ds(base * pitch + row, 8, stride=pitch), :] = sums[
                                base : base + 8, lanes * 128 : (lanes + 1) * 128
                            ]
                return carry

            lax.fori_loop(0, blocks // 16, rows, 0)
            for k in range(len(peers(side, n_low, n_high)[1])):
                encode_rows(side, k, 0, chunk)
                exchange_rows(side, k, chunk).start()

    for side in range(2):
        for k in range(len(peers(side, n_low, n_high)[1])):
            exchange_scale(side, k, 0).start()

    def encode(beam, carry):
        for side in range(2):
            for k in range(len(peers(side, n_low, n_high)[1])):
                for chunk in range(chunks):
                    encode_rows(side, k, beam, chunk)
                exchange_scale(side, k, beam).start()
                exchange(side, k, beam).start()
        return carry

    lax.fori_loop(1, n_beams, encode, 0)
    for copy in tables:
        copy.wait()

    def total_of(ref, send_sem, recv_sem):
        return pltpu.make_async_remote_copy(
            src_ref=ref, dst_ref=ref, send_sem=send_sem, recv_sem=recv_sem, device_id=(sub, sta), device_id_type=MESH
        )

    def move(beam, k):
        return pltpu.make_async_remote_copy(
            src_ref=ready.at[sub_peer(k), beam],
            dst_ref=middle.at[beam, sub],
            send_sem=move_send.at[k - 1],
            recv_sem=move_recv.at[beam],
            device_id=(sub_peer(k), sta),
            device_id_type=MESH,
        )

    def move_peak(k):
        return pltpu.make_async_remote_copy(
            src_ref=ready_peak,
            dst_ref=middle_peak.at[sub],
            send_sem=peak_send,
            recv_sem=peak_recv,
            device_id=(sub_peer(k), sta),
            device_id_type=MESH,
        )

    def forward(beam, k):
        return pltpu.make_async_remote_copy(
            src_ref=middle.at[beam, :, sta_peer(k)],
            dst_ref=out_ref.at[sta, beam],
            send_sem=pass_send.at[k - 1],
            recv_sem=pass_recv.at[k - 1],
            device_id=(sub, sta_peer(k)),
            device_id_type=MESH,
        )

    def forward_peak(k):
        return pltpu.make_async_remote_copy(
            src_ref=middle_peak,
            dst_ref=peak_ref.at[sta],
            send_sem=last_send,
            recv_sem=last_recv,
            device_id=(sub, sta_peer(k)),
            device_id_type=MESH,
        )

    def keep(beam):
        return pltpu.make_async_copy(middle.at[beam, :, sta], out_ref.at[sta, beam], own_sem.at[0])

    lag = 5

    def spread(beam, carry):
        total_of(middle.at[beam, pl.ds(0, n_sub - 1)], move_send.at[0], move_recv.at[beam]).wait_recv()
        for k in range(1, n_sta):
            forward(beam, k).start()
        keep(beam).start()
        return carry

    def finish(beam, carry):
        for side in range(2):
            for k in range(len(peers(side, n_low, n_high)[1])):
                exchange_scale(side, k, beam).wait_recv()
                exchange(side, k, beam).wait_recv()
        quarters = []
        for part in range(2):
            for side in range(2):
                pair = []
                for lanes in range(2):
                    total = piece(side, 0, part, beam, lanes)
                    for k in range(len(peers(side, n_low, n_high)[1])):
                        pieces = []
                        for chunk in range(chunks):
                            tall = half // chunks
                            ceiling = scale_in[side][k, beam, lanes, chunk : chunk + 1, :]
                            rows = pl.ds(chunk * tall, tall)
                            pieces.append(dequantize(landed[side][k, beam, part, lanes, rows, :], ceiling))
                        total = total + jnp.concatenate(pieces, axis=0)
                    pair.append(total)
                quarters.append(jnp.concatenate(pair, axis=1))
        x = jnp.concatenate(quarters, axis=0)
        series = disperse(x, chirp[beam, 0], chirp[beam, 1], left_ref, right_ref, twist_ref)
        for part in range(2):
            for lanes in range(2):
                flat[part, pl.ds(lanes, root, 2), :] = series[
                    part * root : (part + 1) * root, lanes * half : (lanes + 1) * half
                ]
        values = [flat[part] for part in range(2)]
        ceiling = jnp.max(jnp.maximum(jnp.abs(values[0]), jnp.abs(values[1])), axis=0, keepdims=True)
        ready_peak[pl.ds(beam, 1), :] = ceiling
        for part in range(2):
            ready[:, beam, :, part] = quantize(values[part], ceiling).reshape(n_sub, n_sta, rows_out, half)
        middle[beam, sub] = ready[sub, beam]
        for k in range(1, n_sub):
            move(beam, k).start()

        @pl.when(beam >= lag)
        def _():
            spread(beam - lag, 0)

        return carry

    lax.fori_loop(0, n_beams, finish, 0)
    middle_peak[sub] = ready_peak[...]
    for k in range(1, n_sub):
        move_peak(k).start()

    lax.fori_loop(max(n_beams - lag, 0), n_beams, spread, 0)
    arrived = middle_peak.at[pl.ds(0, n_sub - 1)]
    total_of(arrived, peak_send, peak_recv).wait_recv()
    for k in range(1, n_sta):
        forward_peak(k).start()
    own_peak = pltpu.make_async_copy(middle_peak, peak_ref.at[sta], own_sem.at[1])
    own_peak.start()

    for side in range(2):
        whole = volt_ref.at[pl.ds(side * chunks * blocks, chunks * blocks)]
        for k in range(len(peers(side, n_low, n_high)[0])):
            total_of(whole, gather_send[side].at[k], gather_send[side].at[k]).wait_send()
        for k in range(len(peers(side, n_low, n_high)[1])):
            total_of(codes[side].at[k], sum_send[side].at[k], sum_send[side].at[k]).wait_send()
            total_of(scale[side].at[k], scale_send[side].at[k], scale_send[side].at[k]).wait_send()
    for k in range(1, n_sub):
        total_of(ready.at[sub_peer(k)], move_send.at[k - 1], move_send.at[k - 1]).wait_send()
    total_of(arrived, peak_send, peak_recv).wait_send()
    pltpu.make_async_copy(middle.at[:, :, sta], out_ref.at[sta], own_sem.at[0]).wait()
    own_peak.wait()
    for k in range(1, n_sta):
        total_of(middle.at[:, :, sta_peer(k)], pass_send.at[k - 1], pass_recv.at[k - 1]).wait_send()
        total_of(out_ref.at[sta_peer(k)], pass_send.at[k - 1], pass_recv.at[k - 1]).wait_recv()
    others = peak_ref.at[pl.ds(0, n_sta - 1)]
    total_of(others, last_send, last_recv).wait()


def make_series(dm_index, delays, volts, weights, n_low, n_high, n_sub, root):
    depth, blocks = 2 * volts.shape[1], volts.shape[2] // 128
    spread_rows = depth + 4
    chunks = 8
    n_beams = dm_index.shape[0]
    half = root // 2
    n_sta = n_low * n_high
    rows_out = 2 * root // (n_sub * n_sta)
    tables = dft_tables(root)
    vmem = pl.BlockSpec(memory_space=pltpu.VMEM)
    hbm = pl.BlockSpec(memory_space=pltpu.HBM)
    pitch = half + 4
    dma = pltpu.SemaphoreType.DMA
    groups = ((n_low, n_high), (n_high, n_low))
    per_side = lambda make: [make(*group) for group in groups]
    return pl.pallas_call(
        functools.partial(series_kernel, n_low, n_high, chunks),
        in_specs=[*[pl.BlockSpec(memory_space=pltpu.SMEM)] * 2, hbm, vmem, *[hbm] * 3],
        out_specs=(hbm, hbm),
        out_shape=(
            jax.ShapeDtypeStruct((n_sta, n_beams, n_sub, 2, rows_out, 128), jnp.int16),
            jax.ShapeDtypeStruct((n_sta, n_sub, n_beams, 128), jnp.float32),
        ),
        scratch_shapes=[
            *per_side(lambda g, r: pltpu.VMEM((g - 1, blocks // 2, depth, 128), jnp.bfloat16)),
            *per_side(lambda g, r: pltpu.VMEM((2, r * 2 * n_beams * pitch, 128), jnp.float32)),
            *per_side(lambda g, r: pltpu.VMEM((r - 1, n_beams, 2, 2, half, 128), jnp.int16)),
            *per_side(lambda g, r: pltpu.VMEM((r - 1, n_beams, 2, 2, half, 128), jnp.int16)),
            *per_side(lambda g, r: pltpu.VMEM((r - 1, n_beams, 2, 8, 128), jnp.float32)),
            *per_side(lambda g, r: pltpu.VMEM((r - 1, n_beams, 2, 8, 128), jnp.float32)),
            *per_side(lambda g, r: dma((g - 1,))),
            *per_side(lambda g, r: dma((g - 1, chunks))),
            *per_side(lambda g, r: dma((r - 1,))),
            *per_side(lambda g, r: dma((r - 1, n_beams))),
            *per_side(lambda g, r: dma((r - 1,))),
            *per_side(lambda g, r: dma((r - 1, n_beams))),
            pltpu.VMEM((n_beams, 2, root, root), jnp.float32),
            pltpu.VMEM((2, 2 * root, 128), jnp.float32),
            pltpu.VMEM((n_sub, n_beams, n_sta, 2, rows_out, 128), jnp.int16),
            pltpu.VMEM((n_beams, 128), jnp.float32),
            pltpu.VMEM((n_beams, n_sub, n_sta, 2, rows_out, 128), jnp.int16),
            pltpu.VMEM((n_sub, n_beams, 128), jnp.float32),
            dma((n_sub - 1,)),
            dma((n_beams,)),
            dma,
            dma,
            dma((n_sta - 1,)),
            dma((n_sta - 1,)),
            dma,
            dma,
            dma((2,)),
            *per_side(lambda g, r: pltpu.VMEM((r * 2 * n_beams, g * depth), jnp.float32)),
            pltpu.VMEM((blocks, depth, 128), jnp.bfloat16),
            pltpu.VMEM(((blocks + 16) * spread_rows, 128), jnp.float32),
            pltpu.VMEM((blocks // 2 // chunks * spread_rows, 128), jnp.float32),
            pltpu.VMEM((2, weights.shape[1], 128), jnp.float32),
            *[pltpu.VMEM(table.shape, table.dtype) for table in tables],
            dma((3,)),
            pltpu.VMEM(volts.shape, volts.dtype),
            dma((4,)),
        ],
        compiler_params=pltpu.CompilerParams(
            collective_id=0, has_side_effects=True, vmem_limit_bytes=60 * 1024 * 1024
        ),
        cost_estimate=pl.CostEstimate(
            flops=8 * n_beams * depth * blocks * 128, bytes_accessed=2 * volts.size, transcendentals=0
        ),
    )(dm_index[:, 0], delays, volts, weights, *tables)


def unpack_kernel(codes_ref, peak_ref, out_ref, power_ref):
    n_sub, _, n_beams = out_ref.shape[:3]
    for owner in range(codes_ref.shape[0]):
        for beam in range(codes_ref.shape[1]):
            at = owner * codes_ref.shape[1] + beam
            power = jnp.zeros(power_ref.shape[1:], jnp.float32)
            for sub in range(n_sub):
                ceiling = peak_ref[owner, sub, beam : beam + 1, :]
                for part in range(2):
                    values = dequantize(codes_ref[owner, beam, sub, part], ceiling)
                    out_ref[sub, part, at] = values
                    power = power + values * values
            power_ref[at] = power * (1.0 / n_sub)


def unpack_series(codes, peak):
    n_sta, n_beams, n_sub, _, rows, lanes = codes.shape
    group = n_sta // 2
    return pl.pallas_call(
        unpack_kernel,
        grid=(n_sta // group,),
        in_specs=[
            pl.BlockSpec((group, n_beams, n_sub, 2, rows, lanes), lambda i: (i, 0, 0, 0, 0, 0)),
            pl.BlockSpec((group, n_sub, n_beams, lanes), lambda i: (i, 0, 0, 0)),
        ],
        out_specs=[
            pl.BlockSpec((n_sub, 2, group * n_beams, rows, lanes), lambda i: (0, 0, i, 0, 0)),
            pl.BlockSpec((group * n_beams, rows, lanes), lambda i: (i, 0, 0)),
        ],
        out_shape=[
            jax.ShapeDtypeStruct((n_sub, 2, n_sta * n_beams, rows, lanes), jnp.float32),
            jax.ShapeDtypeStruct((n_sta * n_beams, rows, lanes), jnp.float32),
        ],
    )(codes, peak)


def shards(voltages, beam_weights, station_delays, dm_index):
    sub_dev = voltages.shape[0]
    total_len = voltages.shape[3]
    local_beams = dm_index.shape[0]
    trials = dm_index.shape[1]
    root_len = int(round(total_len**0.5))
    n_sub = lax.axis_size("sub")
    n_sta = lax.axis_size("sta")
    assert sub_dev == 1 and trials == 1 and root_len * root_len == total_len
    n_low = 2 if n_sta % 2 == 0 else 1
    n_high = n_sta // n_low
    codes, peak = make_series(
        dm_index, station_delays, voltages[0], beam_weights[0], n_low, n_high, n_sub, root_len
    )
    moved, intensity = unpack_series(codes, peak)
    return (moved.reshape(*moved.shape[:3], 1, -1), intensity.reshape(intensity.shape[0], 1, -1))


def solution(mesh):
    return jax.shard_map(
        shards,
        mesh=mesh,
        in_specs=(
            P("sub", None, "sta", None),
            P("sub", None, None, None),
            P("sta"),
            P("sta", None),
        ),
        out_specs=(P(None, None, None, None, ("sub", "sta")), P(None, None, ("sub", "sta"))),
        check_vma=False,
    )
```
